512 devices in a mesh: role: 4 (over z_lo, core), grp: 32 (over z_hi, y), rep: 4 (over x).
Axes of the slice: x: 4, y: 8, z: 8 (z_hi: 4, z_lo: 2; z = z_hi * 2 + z_lo), core: 2. Of those that a mesh axis runs over, the one named last changes fastest.
Arguments:
- facets: bfloat16 [4, 2, 4096, 4096], P('role', None, ('grp', 'rep')), may hold values from -6 to 6
- taper: float32 [4, 4096], P('role'), may hold values from 0.3 to 1.5
- kernel: float32 [8], replicated, may hold values from 0.1 to 0.5
- observed: float32 [2, 128, 16, 512], P(None, ('role', 'grp'), 'rep'), may hold values from -6 to 6
- patch_pos: int32 [128, 16], P(('role', 'grp'), 'rep'), may hold values from 0 to 23, as said below
- counts: int32 [128, 16], P(('role', 'grp'), 'rep'), may hold values from 1 to 512, 5120 in all within a row
- vis_u: int32 [128, 16, 512], P(('role', 'grp'), 'rep'), may hold values from 0 to 24
- vis_v: int32 [128, 16, 512], P(('role', 'grp'), 'rep'), may hold values from 0 to 24
Outputs:
- residual_vis: float32 [2, 128, 16, 512], P(None, ('role', 'grp'), 'rep')
- returned: bfloat16 [2, 128, 128, 128], P(None, None, ('grp', 'rep'))
The draws below stay inside these ranges and needn't reach their ends.
Inputs may be any that keep to these rules, and one draw needn't show every extreme that they name: Visibility slots v < counts are live, the rest are padding; the counts of one subgrid's patches sum to 5120 and one of them equals 512. `patch_pos`: split the patches of a subgrid into 4 aligned runs of 4; in each run the first patch covers a block in the first column of blocks and the second a block in the last column of blocks, the others any block.
All inputs are finite; a program needn't handle non-finite values. No bound on the sum of `counts` on one device may be relied on, other than what follows from the above.
Results may differ from the reference program's by a relative error of at most 0.014.
Values may be sent and summed in bfloat16 or wider, within the bound.
A program may use at most 64 MiB of HBM per device.

```python
import math
import jax
import jax.numpy as jnp
import numpy as np
from jax import lax

F = 4096
C = 128
PATCH = 32
EDGE = 32
KW = 8
KMAX = 512
NP = 16
FACETS = 4
NSX = 128
N_REP = 4


def draw_patch_pos(key, part):
    col_blocks = (C + 2 * EDGE) // PATCH
    row_blocks = C // PATCH
    key_rows = jax.random.fold_in(key, 11)
    key_cols = jax.random.fold_in(key, 23)
    row_pick = jax.random.randint(key_rows, (NSX, NP), 0, row_blocks, dtype=jnp.int32)
    col_pick = jax.random.randint(key_cols, (NSX, NP), 0, col_blocks, dtype=jnp.int32)
    local_index = (jnp.arange(NP, dtype=jnp.int32) % (NP // N_REP))[None, :]
    col_final = jnp.where(local_index == 0, 0, jnp.where(local_index == 1, col_blocks - 1, col_pick))
    return (row_pick * col_blocks + col_final).astype(jnp.int32)


def plant(values, key, least, top_value):
    extent = values.shape
    spot = [jax.random.randint(jax.random.fold_in(key, axis), (), 0, extent[axis]) for axis in range(len(extent))]
    values = values.at[tuple(spot)].set(least)
    longest = extent.index(max(extent))
    spot[longest] = (spot[longest] + 1) % extent[longest]
    return values.at[tuple(spot)].set(top_value)


def steps_of(key, extent, cuts, least, top_value):
    def one(dim, blocks):
        steps = jax.random.uniform(jax.random.fold_in(jax.random.fold_in(key, 6), dim), (blocks,), jnp.float32, least / len(cuts), top_value / len(cuts))
        return jnp.repeat(jnp.exp(steps), extent[dim] // blocks).reshape((-1,) + (1,) * (len(extent) - dim - 1))

    gain = one(*cuts[0])
    for cut in cuts[1:]:
        gain = gain * one(*cut)
    return gain


def profile(number_of, total, bound, slope):
    weights = [(1 << 20) // math.isqrt(rank ** slope) + 1 for rank in range(2, number_of + 1)]
    surplus, holding = total - bound - (number_of - 1), [1] * (number_of - 1)
    while surplus > 0:
        candidates = [i for i in range(number_of - 1) if holding[i] < bound]
        pool, left = sum([weights[i] for i in candidates]), surplus
        for i in candidates:
            addition = min(bound - holding[i], max(1, left * weights[i] // pool), surplus)
            holding[i] = holding[i] + addition
            surplus = surplus - addition
    return np.array([bound] + holding)


def uneven_parts(rng, number_of, total, bound, lean):
    if number_of == 2:
        one = jax.random.randint(rng, (), max(1, total - bound), min(bound, total - 1) + 1)
        return jnp.stack([one, total - one])
    sizes = jnp.asarray(profile(number_of, total, bound, lean), jnp.int32)
    twos = (number_of - 1) // 2
    giver, taker = sizes[1:1 + 2 * twos:2], sizes[2:2 + 2 * twos:2]
    margin = jnp.minimum(giver - 1, bound - taker)
    moved = jax.random.randint(jax.random.fold_in(rng, 1), (twos,), 0, 1 << 20) % (margin + 1)
    sizes = sizes.at[1:1 + 2 * twos:2].set(giver - moved).at[2:2 + 2 * twos:2].set(taker + moved)
    return sizes[jax.random.permutation(jax.random.fold_in(rng, 2), number_of)]


def centred(rng, shape, deviation, most, split=(), held_as=jnp.bfloat16):
    entries = jax.random.normal(rng, shape, jnp.float32) * deviation
    if len(split) > 0:
        entries = steps_of(rng, shape, split, -0.22, 0.18) * entries
    return jnp.clip(entries, min=-most, max=most).astype(held_as)


def setup_inputs(seed: int = 0) -> dict:
    seeds = jax.random.split(jax.random.key(seed), 9)
    return {
        "facets": centred(seeds[0], (FACETS, 2, F, F), 1.0, 6.0, ((0, 4), (2, 128))),
        "taper": jnp.clip(0.3 + 1.2 * jax.random.uniform(seeds[1], (FACETS, F), jnp.float32) ** steps_of(seeds[1], (FACETS, F), ((0, 4),), -0.2, 0.2), 0.3, 1.5),
        "kernel": jnp.clip(jax.random.uniform(seeds[2], (KW,), jnp.float32, 0.1, 0.5), 0.1, 0.5),
        "observed": centred(seeds[3], (2, NSX, NP, KMAX), 1.0, 6.0, ((1, 128), (2, 4)), jnp.float32),
        "patch_pos": draw_patch_pos(jax.random.fold_in(seeds[8], 71), 0),
        "counts": jax.vmap(lambda own: uneven_parts(own, NP, NP * KMAX * 5 // 8, KMAX, 2))(jax.random.split(seeds[5], NSX)).reshape((NSX, NP)).astype(jnp.int32),
        "vis_u": plant(jax.random.randint(seeds[6], (NSX, NP, KMAX), 0, PATCH - KW + 1), jax.random.fold_in(seeds[6], 1), 0, PATCH - KW).astype(jnp.int32),
        "vis_v": plant(jax.random.randint(seeds[7], (NSX, NP, KMAX), 0, PATCH - KW + 1), jax.random.fold_in(seeds[7], 1), 0, PATCH - KW).astype(jnp.int32),
    }


def phases(frequency, length):
    columns = jnp.arange(length, dtype=jnp.int32)
    product = frequency[:, None] * columns[None, :] % length
    angles = product.astype(jnp.float32) * (2.0 * math.pi / length)
    return (jnp.cos(angles), jnp.sin(angles))

def windowed(frequency, window):
    length = window.shape[0]
    wave_cos, wave_sin = phases(frequency, length)
    scale_norm = 1.0 / math.sqrt(length)
    table_re = (window[None, :] * wave_cos * scale_norm).astype(jnp.bfloat16)
    table_im = (-(window[None, :] * wave_sin) * scale_norm).astype(jnp.bfloat16)
    return (table_re, table_im)

def contract(left, right):
    return lax.dot_general(left, right, (((1,), (1,)), ((), ())), preferred_element_type=jnp.float32)

def project(table_re, table_im, data_re, data_im):
    part_re = contract(table_re, data_re) - contract(table_im, data_im)
    part_im = contract(table_re, data_im) + contract(table_im, data_re)
    return (part_re, part_im)

def modulate(part_re, part_im, wave_cos, wave_sin):
    mod_re = (part_re * wave_cos + part_im * wave_sin).astype(jnp.bfloat16)
    mod_im = (part_im * wave_cos - part_re * wave_sin).astype(jnp.bfloat16)
    return (mod_re, mod_im)

def kernel_rows(offsets, kernel):
    cell_index = jnp.arange(PATCH, dtype=jnp.int32)
    distance = cell_index[None, :, None] - offsets[:, None, :]
    result = jnp.zeros(distance.shape, jnp.float32)
    for position in range(KW):
        result = result + kernel[position] * (distance == position).astype(jnp.float32)
    return result

def degrid(widened, patch_pos, counts, vis_u, vis_v, observed, kernel):
    high = lax.Precision.HIGHEST
    row_blocks = widened.shape[1] // PATCH
    col_blocks = widened.shape[2] // PATCH
    blocks = widened.reshape(2, row_blocks, PATCH, col_blocks, PATCH).transpose(0, 1, 3, 2, 4)
    blocks = blocks.reshape(2, row_blocks * col_blocks, PATCH, PATCH)
    selected = jnp.take(blocks, patch_pos, axis=1).astype(jnp.float32)
    rows_u = kernel_rows(vis_u, kernel)
    rows_v = kernel_rows(vis_v, kernel)
    partial_value = jnp.einsum('cpab,pav->cpbv', selected, rows_u, precision=high)
    predicted = jnp.einsum('cpbv,pbv->cpv', partial_value, rows_v, precision=high)
    live_mask = (jnp.arange(observed.shape[-1], dtype=jnp.int32)[None, :] < counts[:, None]).astype(jnp.float32)
    residual = (observed - predicted) * live_mask[None]
    weighted = residual[:, :, None, :] * rows_v[None]
    gridded = jnp.einsum('pav,cpbv->cpab', rows_u, weighted, precision=high)
    one_hot = (patch_pos[:, None] == jnp.arange(row_blocks * col_blocks, dtype=jnp.int32)[None, :]).astype(jnp.float32)
    placed = jnp.einsum('pq,cpab->cqab', one_hot, gridded, precision=high)
    regrid = placed.reshape(2, row_blocks, col_blocks, PATCH, PATCH).transpose(0, 1, 3, 2, 4)
    return (residual, regrid.reshape(2, widened.shape[1], widened.shape[2]))

def reference(facets, taper, kernel, observed, patch_pos, counts, vis_u, vis_v):
    row_freq = jnp.arange(C, dtype=jnp.int32)

    def section_one(pair):
        facet, window = pair
        table_re, table_im = windowed(row_freq, window)
        part_re, part_im = project(table_re, table_im, facet[0], facet[1])
        return jnp.stack([part_re, part_im]).astype(jnp.bfloat16)
    parts = lax.map(section_one, (facets, taper))
    base_re, base_im = windowed(jnp.arange(C, dtype=jnp.int32), jnp.ones((F,), jnp.float32))

    def section_two(column):
        shift_freq = (column * (F // NSX)).astype(jnp.int32).reshape(1)
        wave_cos, wave_sin = phases(shift_freq, F)
        total = jnp.zeros((2, C, C), jnp.float32)
        for facet in range(FACETS):
            window = taper[facet][None, :]
            mod_re, mod_im = modulate(parts[facet, 0].astype(jnp.float32), parts[facet, 1].astype(jnp.float32), window * wave_cos, window * wave_sin)
            q_re, q_im = project(mod_re, mod_im, base_re, base_im)
            contrib = jnp.stack([q_re, q_im]).astype(jnp.bfloat16)
            total = total + contrib.astype(jnp.float32)
        return total.astype(jnp.bfloat16)
    subs = lax.map(section_two, jnp.arange(NSX, dtype=jnp.int32))
    zeros_col = jnp.zeros((1, 2, C, C), jnp.bfloat16)
    left_nb = jnp.concatenate([zeros_col, subs[:-1]], axis=0)[..., C - EDGE:]
    right_nb = jnp.concatenate([subs[1:], zeros_col], axis=0)[..., :EDGE]
    widened = jnp.concatenate([left_nb, subs, right_nb], axis=-1)
    flat_obs = observed.transpose(1, 0, 2, 3)

    def one_subgrid(items):
        wide, pos, cnt, uu, vv, obs = items
        return degrid(wide, pos, cnt, uu, vv, obs, kernel)
    residual, regrid = lax.map(one_subgrid, (widened, patch_pos, counts, vis_u, vis_v, flat_obs))
    residual_vis = residual.transpose(1, 0, 2, 3)
    center = regrid[..., EDGE:EDGE + C]
    zeros_edge = jnp.zeros((1, 2, C, EDGE), jnp.float32)
    from_left = jnp.concatenate([zeros_edge, regrid[:-1, :, :, EDGE + C:]], axis=0)
    from_right = jnp.concatenate([regrid[1:, :, :, :EDGE], zeros_edge], axis=0)
    resid = center.at[..., :EDGE].add(from_left).at[..., C - EDGE:].add(from_right)
    resid = resid.astype(jnp.bfloat16)
    returned = resid.transpose(1, 0, 2, 3)
    return (residual_vis, returned)
```

```python
import math

import jax
import jax.numpy as jnp
import numpy as np
from jax import lax
from jax.experimental import pallas as pl
from jax.experimental.pallas import tpu as pltpu
from jax.sharding import PartitionSpec as P

F = 4096
C = 128
PATCH = 32
KW = 8
NP_LOCAL = 4
KMAX = 512
ROLES = 4
GRPS = 32
REPS = 4
MESH = pl.DeviceIdType.MESH
bf16 = jnp.bfloat16
f32 = jnp.float32


def row_order():
    place = np.arange(C)
    return 4 * (place % GRPS) + place // GRPS


def tables():
    turn = 2.0 * math.pi
    row = row_order()
    cell = np.arange(128)
    block = np.arange(32)
    angle = turn * ((cell[:, None] * row[None, :]) % F) / F
    near = np.concatenate([np.cos(angle), -np.sin(angle)], axis=1)
    angle = turn * ((block[:, None] * row[None, :]) % 32) / 32
    far = np.concatenate([np.cos(angle), -np.sin(angle)], axis=1) / math.sqrt(F)
    angle = turn * ((cell[:, None] * block[None, :]) % 32) / 32
    cos, sin = np.cos(angle), np.sin(angle)
    first = np.block([[cos, sin], [-sin, cos]])
    angle = turn * ((cell[:, None] * cell[None, :]) % F) / F
    twist = np.concatenate([np.cos(angle), np.sin(angle)], axis=1)
    angle = turn * ((cell[:, None] * cell[None, :]) % 128) / 128
    cos, sin = np.cos(angle) / math.sqrt(F), np.sin(angle) / math.sqrt(F)
    second = np.concatenate([cos, sin, -sin, cos], axis=1)
    return (
        jnp.asarray(near, bf16),
        jnp.asarray(far, f32),
        jnp.asarray(first, bf16),
        jnp.asarray(twist, f32),
        jnp.asarray(second, bf16),
    )


def mm(left, right):
    return lax.dot_general(left, right, (((1,), (0,)), ((), ())), preferred_element_type=f32)


def mm_t(left, right):
    return lax.dot_general(left, right, (((1,), (1,)), ((), ())), preferred_element_type=f32)


def put_rows(ref, value):
    for i in range(value.shape[0]):
        ref[i, 0:1, :] = value[i : i + 1, :]


def get_rows(ref):
    return ref[...].reshape(ref.shape[0], ref.shape[2])


def body(
    facets, taper, taps, observed, patch_pos, counts, vis_u, vis_v,
    near, far, first, twist, second,
    residual, returned,
    x_out, x_in, q_out, q_in, u_out, u_in, s_out, s_in,
    y_out, y_in, z_out, z_in, f_out, f_in,
    ku, ku_low, kv, kv_wide, weights,
    sent, got,
):
    role, grp, rep = lax.axis_index("role"), lax.axis_index("grp"), lax.axis_index("rep")

    def near_peer(i):
        return (lax.rem(role + i // REPS, ROLES), grp, lax.rem(rep + i % REPS, REPS))

    def grp_peer(i):
        return lax.rem(grp + i, GRPS)

    barrier = pltpu.get_barrier_semaphore()

    def greet_near(i, _):
        pl.semaphore_signal(barrier, inc=1, device_id=near_peer(i), device_id_type=MESH)
        return 0

    def greet_grp(i, _):
        pl.semaphore_signal(barrier, inc=1, device_id=(role, grp_peer(i), rep), device_id_type=MESH)
        return 0

    lax.fori_loop(1, GRPS, greet_grp, 0)
    lax.fori_loop(1, ROLES * REPS, greet_near, 0)

    def push(src, dst, phase, device):
        pltpu.make_async_remote_copy(
            src_ref=src, dst_ref=dst, send_sem=sent.at[phase], recv_sem=got.at[phase],
            device_id=device, device_id_type=MESH,
        ).start()

    def keep(src, dst, phase):
        pltpu.make_async_copy(src, dst, got.at[phase]).start()

    def arrive(buffer, phase):
        pltpu.make_async_copy(buffer, buffer, got.at[phase]).wait()

    def drain(buffer, count, phase):
        part = buffer.at[pl.ds(0, count)]
        pltpu.make_async_copy(part, part, sent.at[phase]).wait()

    window = taper[...]
    data = [(facets[0, c].astype(f32) * window).astype(bf16) for c in range(2)]
    table = near[...]
    part_re = jnp.zeros((32, C), f32)
    part_im = jnp.zeros((32, C), f32)
    for chunk in range(4):
        blocks = []
        for i in range(8 * chunk, 8 * chunk + 8):
            blocks += [data[0][:, 128 * i : 128 * i + 128], data[1][:, 128 * i : 128 * i + 128]]
        spectrum = mm(jnp.concatenate(blocks, axis=0), table)
        for k in range(8):
            i = 8 * chunk + k
            of_re = spectrum[64 * k : 64 * k + 32]
            of_im = spectrum[64 * k + 32 : 64 * k + 64]
            t_re = of_re[:, :C] - of_im[:, C:]
            t_im = of_re[:, C:] + of_im[:, :C]
            e_re = far[i : i + 1, :C]
            e_im = far[i : i + 1, C:]
            part_re = part_re + (t_re * e_re - t_im * e_im)
            part_im = part_im + (t_re * e_im + t_im * e_re)
    turned = jnp.concatenate([part_re, part_im, part_re, part_im], axis=0).T
    lane = lax.broadcasted_iota(jnp.int32, (1, 128), 1)
    own = taper[:, pl.ds(pl.multiple_of(grp * 128, 128), 128)]
    mine = jnp.zeros((1, 128), f32)
    for r in range(REPS):
        moved = own if r == 0 else pltpu.roll(own, 128 - 32 * r, 1)
        mine = mine + moved * jnp.where(rep == r, 1.0, 0.0)
    mine = jnp.where(lane < 32, mine, 0.0)
    mine = mine + pltpu.roll(mine, 32, 1)
    mine = mine + pltpu.roll(mine, 64, 1)
    turned = turned * mine
    for r in range(REPS):
        low = turned[32 * r : 32 * r + 16]
        high = turned[32 * r + 16 : 32 * r + 32]
        x_out[r] = jnp.where(lane < 64, low, high).astype(bf16)

    pl.semaphore_wait(barrier, GRPS - 1 + ROLES * REPS - 1)

    slot = role * REPS + rep
    keep(x_out.at[rep], x_in.at[slot], 0)

    def send_near(i, _):
        device = near_peer(i)
        push(x_out.at[device[2]], x_in.at[slot], 0, device)
        return 0

    lax.fori_loop(1, ROLES * REPS, send_near, 0)
    arrive(x_in, 0)
    joined = [[jnp.zeros((16, 128), f32) for _ in range(2)] for _ in range(2)]
    for r in range(REPS):
        total = x_in[r].astype(f32)
        for k in range(1, ROLES):
            total = total + x_in[k * REPS + r].astype(f32)
        inside = (lane >= 32 * r) & (lane < 32 * r + 32)
        for h in range(2):
            for c in range(2):
                by = (32 * r - 64 * h - 32 * c) % 128
                moved = total if by == 0 else pltpu.roll(total, by, 1)
                joined[h][c] = jnp.where(inside, moved, joined[h][c])
    put_rows(q_out, jnp.concatenate([jnp.concatenate(joined[h], axis=1) for h in range(2)], axis=0))

    def swap(out, into, phase):
        keep(out.at[grp], into.at[grp], phase)

        def send(i, _):
            to = grp_peer(i)
            push(out.at[to], into.at[grp], phase, (role, to, rep))
            return 0

        lax.fori_loop(1, GRPS, send, 0)

    swap(q_out, q_in, 1)

    sub = role * GRPS + grp
    place = lax.broadcasted_iota(jnp.int32, (PATCH, KMAX), 0)
    row_in_patch = 4 * (place % 8) + place // 8
    has_left = jnp.where(sub > 0, 1, 0)
    has_right = jnp.where(sub < ROLES * GRPS - 1, 1, 0)

    def block_of(p):
        position = jnp.full((1, KMAX), patch_pos[0, p], jnp.int32)
        row_block = (
            jnp.where(position >= 6, 1, 0)
            + jnp.where(position >= 12, 1, 0)
            + jnp.where(position >= 18, 1, 0)
        )
        return row_block, position - 6 * row_block

    for p in range(NP_LOCAL):
        cols = slice(KMAX * p, KMAX * p + KMAX)
        row_block, col_block = block_of(p)
        du = row_in_patch - vis_u[0, p : p + 1, :]
        dv = place - vis_v[0, p : p + 1, :]
        u32 = jnp.zeros((PATCH, KMAX), f32)
        v32 = jnp.zeros((PATCH, KMAX), f32)
        for t in range(KW):
            u32 = jnp.where(du == t, taps[t], u32)
            v32 = jnp.where(dv == t, taps[t], v32)
        kv[:, cols] = v32
        for r in range(REPS):
            rows = u32[8 * r : 8 * r + 8]
            for h in range(2):
                pair = jnp.concatenate(
                    [jnp.where(row_block == 2 * h + k, rows, 0.0) for k in range(2)], axis=0
                )
                at = slice(32 * r + 16 * h, 32 * r + 16 * h + 16)
                ku[at, cols] = pair
                ku_low[at, cols] = pair.astype(bf16)
        for u in range(4):
            chosen = jnp.where(col_block == u + 1, 1, 0)
            if u == 2:
                chosen = chosen + jnp.where(col_block == 0, 1, 0) * has_left
            if u == 1:
                chosen = chosen + jnp.where(col_block == 5, 1, 0) * has_right
            kv_wide[32 * u : 32 * u + 32, cols] = jnp.where(chosen > 0, v32, 0.0).astype(bf16)

    arrive(q_in, 1)
    cells = get_rows(q_in)
    stacked = jnp.concatenate([cells[:, :128], cells[:, 128:]], axis=0).astype(bf16)
    mixed = mm(first[...], stacked)
    mixed_re, mixed_im = mixed[:128], mixed[128:]
    cos, sin = twist[:, :128], twist[:, 128:]
    both = jnp.concatenate(
        [mixed_re * cos + mixed_im * sin, mixed_im * cos - mixed_re * sin], axis=1
    ).astype(bf16)
    wave = second[pl.ds(pl.multiple_of(role * GRPS, GRPS), GRPS), :]
    put_rows(
        u_out, jnp.concatenate([mm_t(wave[:, :256], both), mm_t(wave[:, 256:], both)], axis=1)
    )
    swap(u_out, u_in, 2)
    arrive(u_in, 2)

    s_out[0] = get_rows(u_in).astype(bf16)
    keep(s_out.at[0], s_in.at[rep], 3)

    def send_rows(i, _):
        push(s_out.at[0], s_in.at[rep], 3, (role, grp, lax.rem(rep + i, REPS)))
        return 0

    lax.fori_loop(1, REPS, send_rows, 0)
    arrive(s_in, 3)

    rows = [s_in[r] for r in range(REPS)]
    grid_cells = jnp.concatenate(
        [row[:, :128] for row in rows] + [row[:, 128:] for row in rows], axis=0
    )
    slots = lax.broadcasted_iota(jnp.int32, (1, KMAX), 1)
    for p in range(NP_LOCAL):
        cols = slice(KMAX * p, KMAX * p + KMAX)
        _, col_block = block_of(p)
        live = slots < jnp.full((1, KMAX), counts[0, p], jnp.int32)
        along = mm(grid_cells, kv_wide[:, cols])
        ku_p = ku[:, cols]
        kv_p = kv[:, cols]
        for c in range(2):
            predicted = jnp.sum(along[128 * c : 128 * c + 128] * ku_p, axis=0, keepdims=True)
            left_over = jnp.where(live, observed[c, 0, p : p + 1, :] - predicted, 0.0)
            residual[c, 0, p : p + 1, :] = left_over
            weighted = kv_p * left_over
            for u in range(4):
                at = slice(128 * c + 32 * u, 128 * c + 32 * u + 32)
                weights[at, cols] = jnp.where(col_block == u + 1, weighted, 0.0).astype(bf16)
            at = slice(256 + 64 * c, 256 + 64 * c + 32)
            weights[at, cols] = jnp.where(col_block == 0, weighted, 0.0).astype(bf16)
            at = slice(288 + 64 * c, 288 + 64 * c + 32)
            weights[at, cols] = jnp.where(col_block == 5, weighted, 0.0).astype(bf16)
    gridded = mm_t(ku_low[...], weights[...])
    for r in range(REPS):
        y_out[r] = gridded[32 * r : 32 * r + 32].astype(bf16)

    keep(y_out.at[rep], y_in.at[rep], 4)

    def send_gridded(i, _):
        to = lax.rem(rep + i, REPS)
        push(y_out.at[to], y_in.at[rep], 4, (role, grp, to))
        return 0

    lax.fori_loop(1, REPS, send_gridded, 0)
    arrive(y_in, 4)
    total = y_in[0].astype(f32)
    for r in range(1, REPS):
        total = total + y_in[r].astype(f32)
    put_rows(z_out, total)
    swap(z_out, z_in, 5)
    arrive(z_in, 5)
    f_out[0] = get_rows(z_in).astype(bf16)
    keep(f_out.at[0], f_in.at[role], 6)

    def send_owned(i, _):
        push(f_out.at[0], f_in.at[role], 6, (lax.rem(role + i, ROLES), grp, rep))
        return 0

    lax.fori_loop(1, ROLES, send_owned, 0)
    arrive(f_in, 6)

    owned = jnp.concatenate([f_in[k] for k in range(ROLES)], axis=0).astype(f32)
    edges = owned[:, 256:]
    column = lax.broadcasted_iota(jnp.int32, (C, 128), 1)
    subgrid = lax.broadcasted_iota(jnp.int32, (C, 128), 0)
    for c in range(2):
        side = pltpu.roll(edges, 96 if c == 0 else 32, 1)
        from_left = jnp.where((column < 32) & (subgrid > 0), pltpu.roll(side, 1, 0), 0.0)
        from_right = jnp.where((column >= 96) & (subgrid < C - 1), pltpu.roll(side, C - 1, 0), 0.0)
        returned[c] = (owned[:, 128 * c : 128 * c + 128] + from_left + from_right).astype(bf16)

    drain(x_in, 15, 0)
    drain(q_in, 31, 1)
    drain(u_in, 31, 2)
    drain(s_in, 3, 3)
    drain(y_in, 3, 4)
    drain(z_in, 31, 5)
    drain(f_in, 3, 6)


def local(facets, taper, kernel, observed, patch_pos, counts, vis_u, vis_v):
    vmem = pl.BlockSpec(memory_space=pltpu.VMEM)
    smem = pl.BlockSpec(memory_space=pltpu.SMEM)
    residual, returned = pl.pallas_call(
        body,
        out_shape=(
            jax.ShapeDtypeStruct((2, 1, NP_LOCAL, KMAX), f32),
            jax.ShapeDtypeStruct((2, C, C), bf16),
        ),
        in_specs=[vmem, vmem, smem, vmem, smem, smem, vmem, vmem] + [vmem] * 5,
        out_specs=(vmem, vmem),
        scratch_shapes=[
            pltpu.VMEM((REPS, 16, 128), bf16),
            pltpu.VMEM((ROLES * REPS, 16, 128), bf16),
            pltpu.VMEM((GRPS, 1, 256), f32),
            pltpu.VMEM((GRPS, 1, 256), f32),
            pltpu.VMEM((GRPS, 1, 256), f32),
            pltpu.VMEM((GRPS, 1, 256), f32),
            pltpu.VMEM((1, 32, 256), bf16),
            pltpu.VMEM((REPS, 32, 256), bf16),
            pltpu.VMEM((REPS, 32, 384), bf16),
            pltpu.VMEM((REPS, 32, 384), bf16),
            pltpu.VMEM((GRPS, 1, 384), f32),
            pltpu.VMEM((GRPS, 1, 384), f32),
            pltpu.VMEM((1, 32, 384), bf16),
            pltpu.VMEM((ROLES, 32, 384), bf16),
            pltpu.VMEM((C, NP_LOCAL * KMAX), f32),
            pltpu.VMEM((C, NP_LOCAL * KMAX), bf16),
            pltpu.VMEM((PATCH, NP_LOCAL * KMAX), f32),
            pltpu.VMEM((C, NP_LOCAL * KMAX), bf16),
            pltpu.VMEM((384, NP_LOCAL * KMAX), bf16),
            pltpu.SemaphoreType.DMA((7,)),
            pltpu.SemaphoreType.DMA((7,)),
        ],
        compiler_params=pltpu.CompilerParams(collective_id=0, has_side_effects=True),
        name="cycle",
    )(facets, taper, kernel, observed, patch_pos, counts, vis_u, vis_v, *tables())
    return residual, returned.reshape(2, C, 1, C)


def solution(mesh):
    both = ("role", "grp")
    return jax.shard_map(
        local,
        mesh=mesh,
        in_specs=(
            P("role", None, ("grp", "rep"), None),
            P("role", None),
            P(),
            P(None, both, "rep", None),
            P(both, "rep"),
            P(both, "rep"),
            P(both, "rep", None),
            P(both, "rep", None),
        ),
        out_specs=(P(None, both, "rep", None), P(None, None, ("grp", "rep"), None)),
        check_vma=False,
    )
```

```python
import math

import jax
import jax.numpy as jnp
import numpy as np
from jax import lax
from jax.experimental import pallas as pl
from jax.experimental.pallas import tpu as pltpu
from jax.sharding import PartitionSpec as P

F = 4096
C = 128
PATCH = 32
KW = 8
NP_LOCAL = 4
KMAX = 512
ROLES = 4
GRPS = 32
REPS = 4
NEAR = ROLES * REPS
FAR = 13
MESH = pl.DeviceIdType.MESH
bf16 = jnp.bfloat16
f32 = jnp.float32


def row_order():
    place = np.arange(C)
    return 4 * (place % GRPS) + place // GRPS


def tables():
    turn = 2.0 * math.pi
    row = row_order()
    cell = np.arange(128)
    block = np.arange(32)
    angle = turn * ((cell[:, None] * row[None, :]) % F) / F
    near = np.concatenate([np.cos(angle), -np.sin(angle)], axis=1)
    angle = turn * ((block[:, None] * row[None, :]) % 32) / 32
    far = np.concatenate([np.cos(angle), -np.sin(angle)], axis=1) / math.sqrt(F)
    angle = turn * ((cell[:, None] * block[None, :]) % 32) / 32
    cos, sin = np.cos(angle), np.sin(angle)
    first = np.block([[cos, sin], [-sin, cos]])
    angle = turn * ((cell[:, None] * cell[None, :]) % F) / F
    twist = np.concatenate([np.cos(angle), np.sin(angle)], axis=1)
    angle = turn * ((cell[:, None] * cell[None, :]) % 128) / 128
    cos, sin = np.cos(angle) / math.sqrt(F), np.sin(angle) / math.sqrt(F)
    second = np.stack([np.concatenate([cos, sin], 1), np.concatenate([-sin, cos], 1)], axis=1)
    second = second.reshape(ROLES, GRPS, 2, 256).transpose(1, 0, 2, 3).reshape(GRPS, 8, 256)
    return (
        jnp.asarray(near, bf16),
        jnp.asarray(far, f32),
        jnp.asarray(first, bf16),
        jnp.asarray(twist, f32),
        jnp.asarray(second, bf16),
    )


def mm(left, right):
    return lax.dot_general(left, right, (((1,), (0,)), ((), ())), preferred_element_type=f32)


def mm_t(left, right):
    return lax.dot_general(left, right, (((1,), (1,)), ((), ())), preferred_element_type=f32)


def put_rows(ref, value):
    for i in range(value.shape[0]):
        ref[i, 0:1, :] = value[i : i + 1, :]


def get_rows(ref):
    return ref[...].reshape(ref.shape[0], ref.shape[2])


def body(
    facets_far, taper_far, near_far, far_far, first_far, twist_far, second_far,
    taps_far, observed_far, patch_pos_far, counts_far, vis_u_far, vis_v_far,
    residual, returned,
    facets, taper, near, far, first, twist, second,
    taps, observed, patch_pos, counts, vis_u, vis_v,
    x_out, x_in, q_out, q_in, q_all, u_all, u_out, s_in,
    y_out, y_in, z_out, z_in, f_out, f_in,
    ku, ku_low, kv, kv_wide, weights,
    sent, got, loaded,
):
    role, grp, rep = lax.axis_index("role"), lax.axis_index("grp"), lax.axis_index("rep")

    def near_peer(i):
        return (lax.rem(role + i // REPS, ROLES), grp, lax.rem(rep + i % REPS, REPS))

    def grp_peer(i):
        return lax.rem(grp + i, GRPS)

    inputs = [
        (taper_far, taper), (near_far, near), (far_far, far),
        (first_far, first), (twist_far, twist), (second_far, second),
        (taps_far, taps), (observed_far, observed), (patch_pos_far, patch_pos),
        (counts_far, counts), (vis_u_far, vis_u), (vis_v_far, vis_v),
    ]
    loads = []
    for k in range(4):
        part = pl.ds(1024 * k, 1024)
        loads.append((facets_far.at[0, :, :, part], facets.at[:, :, part]))
    loads = [
        pltpu.make_async_copy(src, dst, loaded.at[k]) for k, (src, dst) in enumerate(loads + inputs)
    ]
    for load in loads[4:7] + loads[:4] + loads[7:]:
        load.start()

    barrier = pltpu.get_barrier_semaphore()

    def greet_near(i, _):
        pl.semaphore_signal(barrier, inc=1, device_id=near_peer(i), device_id_type=MESH)
        return 0

    def greet_grp(i, _):
        pl.semaphore_signal(barrier, inc=1, device_id=(role, grp_peer(i), rep), device_id_type=MESH)
        return 0

    lax.fori_loop(1, GRPS, greet_grp, 0)
    lax.fori_loop(1, NEAR, greet_near, 0)

    def push(src, dst, phase, device):
        pltpu.make_async_remote_copy(
            src_ref=src, dst_ref=dst, send_sem=sent.at[phase], recv_sem=got.at[phase],
            device_id=device, device_id_type=MESH,
        ).start()

    def keep(src, dst, phase):
        pltpu.make_async_copy(src, dst, got.at[phase]).start()

    def arrive(buffer, phase):
        pltpu.make_async_copy(buffer, buffer, got.at[phase]).wait()

    def drain(buffer, count, phase):
        part = buffer.at[pl.ds(0, count)]
        pltpu.make_async_copy(part, part, sent.at[phase]).wait()

    for load in loads[4:7]:
        load.wait()
    table = near[...]
    part_re = jnp.zeros((32, C), f32)
    part_im = jnp.zeros((32, C), f32)
    for chunk in range(4):
        loads[chunk].wait()
        blocks = []
        for i in range(8 * chunk, 8 * chunk + 8):
            at = slice(128 * i, 128 * i + 128)
            blocks += [(facets[c, :, at].astype(f32) * taper[:, at]).astype(bf16) for c in range(2)]
        spectrum = mm(jnp.concatenate(blocks, axis=0), table)
        for k in range(8):
            i = 8 * chunk + k
            of_re = spectrum[64 * k : 64 * k + 32]
            of_im = spectrum[64 * k + 32 : 64 * k + 64]
            t_re = of_re[:, :C] - of_im[:, C:]
            t_im = of_re[:, C:] + of_im[:, :C]
            e_re = far[i : i + 1, :C]
            e_im = far[i : i + 1, C:]
            part_re = part_re + (t_re * e_re - t_im * e_im)
            part_im = part_im + (t_re * e_im + t_im * e_re)
    turned = jnp.concatenate([part_re, part_im, part_re, part_im], axis=0).T
    lane = lax.broadcasted_iota(jnp.int32, (1, 128), 1)
    own = taper[:, pl.ds(pl.multiple_of(grp * 128, 128), 128)]
    mine = jnp.zeros((1, 128), f32)
    for r in range(REPS):
        moved = own if r == 0 else pltpu.roll(own, 128 - 32 * r, 1)
        mine = mine + moved * jnp.where(rep == r, 1.0, 0.0)
    mine = jnp.where(lane < 32, mine, 0.0)
    mine = mine + pltpu.roll(mine, 32, 1)
    mine = mine + pltpu.roll(mine, 64, 1)
    turned = turned * mine
    for k in range(NEAR):
        x_out[k] = turned[8 * k : 8 * k + 8].astype(bf16)

    pl.semaphore_wait(barrier, GRPS + NEAR - 2)

    slot = role * REPS + rep

    def spread(out, into, phase):
        keep(out.at[slot], into.at[slot], phase)

        def send(i, _):
            device = near_peer(i)
            push(out.at[device[0] * REPS + device[2]], into.at[slot], phase, device)
            return 0

        lax.fori_loop(1, NEAR, send, 0)

    spread(x_out, x_in, 0)
    arrive(x_in, 0)
    cell_re = jnp.zeros((8, 128), f32)
    cell_im = jnp.zeros((8, 128), f32)
    for r in range(REPS):
        total = x_in[r].astype(f32)
        for k in range(1, ROLES):
            total = total + x_in[k * REPS + r].astype(f32)
        inside = (lane >= 32 * r) & (lane < 32 * r + 32)
        moved = pltpu.roll(total, 32, 1)
        cell_re = jnp.where(inside, total if r % 2 == 0 else moved, cell_re)
        cell_im = jnp.where(inside, moved if r % 2 == 0 else total, cell_im)
    q_out[0] = jnp.concatenate([cell_re, cell_im], axis=1).astype(bf16)
    keep(q_out.at[0], q_in.at[grp], 1)

    def send_cells(i, _):
        push(q_out.at[0], q_in.at[grp], 1, (role, grp_peer(i), rep))
        return 0

    lax.fori_loop(FAR, GRPS, send_cells, 0)
    lax.fori_loop(1, FAR, send_cells, 0)

    for load in loads[7:]:
        load.wait()
    sub = role * GRPS + grp
    place = lax.broadcasted_iota(jnp.int32, (PATCH, KMAX), 0)
    row_in_patch = 4 * (place % 8) + place // 8
    has_left = jnp.where(sub > 0, 1, 0)
    has_right = jnp.where(sub < ROLES * GRPS - 1, 1, 0)

    def block_of(p):
        position = jnp.broadcast_to(patch_pos[0:1, p : p + 1], (1, KMAX))
        row_block = (
            jnp.where(position >= 6, 1, 0)
            + jnp.where(position >= 12, 1, 0)
            + jnp.where(position >= 18, 1, 0)
        )
        return row_block, position - 6 * row_block

    tap = [jnp.broadcast_to(taps[0:1, t : t + 1], (PATCH, KMAX)) for t in range(KW)]
    for p in range(NP_LOCAL):
        cols = slice(KMAX * p, KMAX * p + KMAX)
        row_block, col_block = block_of(p)
        du = row_in_patch - vis_u[0, p : p + 1, :]
        dv = place - vis_v[0, p : p + 1, :]
        u32 = jnp.zeros((PATCH, KMAX), f32)
        v32 = jnp.zeros((PATCH, KMAX), f32)
        for t in range(KW):
            u32 = jnp.where(du == t, tap[t], u32)
            v32 = jnp.where(dv == t, tap[t], v32)
        kv[:, cols] = v32
        for r in range(REPS):
            rows = u32[8 * r : 8 * r + 8]
            for h in range(2):
                pair = jnp.concatenate(
                    [jnp.where(row_block == 2 * h + k, rows, 0.0) for k in range(2)], axis=0
                )
                at = slice(32 * r + 16 * h, 32 * r + 16 * h + 16)
                ku[at, cols] = pair
                ku_low[at, cols] = pair.astype(bf16)
        for u in range(4):
            chosen = jnp.where(col_block == u + 1, 1, 0)
            if u == 2:
                chosen = chosen + jnp.where(col_block == 0, 1, 0) * has_left
            if u == 1:
                chosen = chosen + jnp.where(col_block == 5, 1, 0) * has_right
            kv_wide[32 * u : 32 * u + 32, cols] = jnp.where(chosen > 0, v32, 0.0).astype(bf16)

    arrive(q_in, 1)
    for k in range(GRPS):
        arrived = q_in[k].astype(f32)
        q_all[8 * k : 8 * k + 8, :] = arrived[:, :128]
        q_all[8 * GRPS + 8 * k : 8 * GRPS + 8 * k + 8, :] = arrived[:, 128:]
    stacked = []
    for k in range(8):
        stacked.append(q_all[pl.ds(k, 2 * GRPS, stride=8), :].astype(bf16))
    mixed = mm(first[...], jnp.concatenate(stacked, axis=1))
    cos, sin = twist[:, :128], twist[:, 128:]
    both = []
    for k in range(8):
        mixed_re = mixed[:128, 128 * k : 128 * k + 128]
        mixed_im = mixed[128:, 128 * k : 128 * k + 128]
        pair = [mixed_re * cos + mixed_im * sin, mixed_im * cos - mixed_re * sin]
        both.append(jnp.concatenate(pair, axis=1).astype(bf16))
    waves = mm_t(second[grp], jnp.concatenate(both, axis=0))
    for k in range(8):
        u_all[8 * k : 8 * k + 8, :] = waves[:, 128 * k : 128 * k + 128]
    for k in range(ROLES):
        pair = [u_all[pl.ds(2 * k + c, 8, stride=8), :] for c in range(2)]
        u_out[k] = jnp.concatenate(pair, axis=1).astype(bf16)

    keep(u_out.at[role], s_in.at[slot], 2)

    def send_rows(i, _):
        device = near_peer(i)
        push(u_out.at[device[0]], s_in.at[slot], 2, device)
        return 0

    lax.fori_loop(1, NEAR, send_rows, 0)
    arrive(s_in, 2)

    rows = jnp.concatenate([s_in[k].astype(f32) for k in range(NEAR)], axis=0).astype(bf16)
    grid_cells = jnp.concatenate([rows[:, :128], rows[:, 128:]], axis=0)
    slots = lax.broadcasted_iota(jnp.int32, (1, KMAX), 1)
    for p in range(NP_LOCAL):
        cols = slice(KMAX * p, KMAX * p + KMAX)
        _, col_block = block_of(p)
        live = slots < jnp.broadcast_to(counts[0:1, p : p + 1], (1, KMAX))
        along = mm(grid_cells, kv_wide[:, cols])
        ku_p = ku[:, cols]
        kv_p = kv[:, cols]
        for c in range(2):
            predicted = jnp.sum(along[128 * c : 128 * c + 128] * ku_p, axis=0, keepdims=True)
            left_over = jnp.where(live, observed[c, 0, p : p + 1, :] - predicted, 0.0)
            residual[c, 0, p : p + 1, :] = left_over
            weighted = kv_p * left_over
            for u in range(4):
                at = slice(128 * c + 32 * u, 128 * c + 32 * u + 32)
                weights[at, cols] = jnp.where(col_block == u + 1, weighted, 0.0).astype(bf16)
            at = slice(256 + 64 * c, 256 + 64 * c + 32)
            weights[at, cols] = jnp.where(col_block == 0, weighted, 0.0).astype(bf16)
            at = slice(288 + 64 * c, 288 + 64 * c + 32)
            weights[at, cols] = jnp.where(col_block == 5, weighted, 0.0).astype(bf16)
    gridded = mm_t(ku_low[...], weights[...])
    for r in range(REPS):
        y_out[r] = gridded[32 * r : 32 * r + 32].astype(bf16)

    keep(y_out.at[rep], y_in.at[rep], 3)

    def send_gridded(i, _):
        to = lax.rem(rep + i, REPS)
        push(y_out.at[to], y_in.at[rep], 3, (role, grp, to))
        return 0

    lax.fori_loop(1, REPS, send_gridded, 0)
    arrive(y_in, 3)
    total = y_in[0].astype(f32)
    for r in range(1, REPS):
        total = total + y_in[r].astype(f32)
    put_rows(z_out, total)
    keep(z_out.at[grp], z_in.at[grp], 4)

    def send_owner(i, _):
        to = grp_peer(i)
        push(z_out.at[to], z_in.at[grp], 4, (role, to, rep))
        return 0

    lax.fori_loop(FAR, GRPS, send_owner, 0)
    lax.fori_loop(1, FAR, send_owner, 0)
    arrive(z_in, 4)
    f_out[0] = get_rows(z_in).astype(bf16)
    keep(f_out.at[0], f_in.at[role], 5)

    def send_owned(i, _):
        push(f_out.at[0], f_in.at[role], 5, (lax.rem(role + i, ROLES), grp, rep))
        return 0

    lax.fori_loop(1, ROLES, send_owned, 0)
    arrive(f_in, 5)

    owned = jnp.concatenate([f_in[k] for k in range(ROLES)], axis=0).astype(f32)
    edges = owned[:, 256:]
    column = lax.broadcasted_iota(jnp.int32, (C, 128), 1)
    subgrid = lax.broadcasted_iota(jnp.int32, (C, 128), 0)
    for c in range(2):
        side = pltpu.roll(edges, 96 if c == 0 else 32, 1)
        from_left = jnp.where((column < 32) & (subgrid > 0), pltpu.roll(side, 1, 0), 0.0)
        from_right = jnp.where((column >= 96) & (subgrid < C - 1), pltpu.roll(side, C - 1, 0), 0.0)
        returned[c] = (owned[:, 128 * c : 128 * c + 128] + from_left + from_right).astype(bf16)

    drain(x_in, NEAR - 1, 0)
    drain(q_in, GRPS - 1, 1)
    drain(s_in, NEAR - 1, 2)
    drain(y_in, REPS - 1, 3)
    drain(z_in, GRPS - 1, 4)
    drain(f_in, ROLES - 1, 5)


def local(facets, taper, kernel, observed, patch_pos, counts, vis_u, vis_v):
    vmem = pl.BlockSpec(memory_space=pltpu.VMEM)
    hbm = pl.BlockSpec(memory_space=pltpu.HBM)
    residual, returned = pl.pallas_call(
        body,
        out_shape=(
            pltpu.VMEM((2, 1, NP_LOCAL, KMAX), f32),
            pltpu.VMEM((2, C, C), bf16),
        ),
        in_specs=[hbm] * 13,
        out_specs=(vmem, vmem),
        scratch_shapes=[
            pltpu.VMEM((2, 32, F), bf16),
            pltpu.VMEM((1, F), f32),
            pltpu.VMEM((128, 256), bf16),
            pltpu.VMEM((32, 256), f32),
            pltpu.VMEM((256, 64), bf16),
            pltpu.VMEM((128, 256), f32),
            pltpu.VMEM((GRPS, 8, 256), bf16),
            pltpu.VMEM((1, KW), f32),
            pltpu.VMEM((2, 1, NP_LOCAL, KMAX), f32),
            pltpu.VMEM((1, NP_LOCAL), jnp.int32),
            pltpu.VMEM((1, NP_LOCAL), jnp.int32),
            pltpu.VMEM((1, NP_LOCAL, KMAX), jnp.int32),
            pltpu.VMEM((1, NP_LOCAL, KMAX), jnp.int32),
            pltpu.VMEM((NEAR, 8, 128), bf16),
            pltpu.VMEM((NEAR, 8, 128), bf16),
            pltpu.VMEM((1, 8, 256), bf16),
            pltpu.VMEM((GRPS, 8, 256), bf16),
            pltpu.VMEM((16 * GRPS, 128), f32),
            pltpu.VMEM((64, 128), f32),
            pltpu.VMEM((ROLES, 8, 256), bf16),
            pltpu.VMEM((NEAR, 8, 256), bf16),
            pltpu.VMEM((REPS, 32, 384), bf16),
            pltpu.VMEM((REPS, 32, 384), bf16),
            pltpu.VMEM((GRPS, 1, 384), f32),
            pltpu.VMEM((GRPS, 1, 384), f32),
            pltpu.VMEM((1, 32, 384), bf16),
            pltpu.VMEM((ROLES, 32, 384), bf16),
            pltpu.VMEM((C, NP_LOCAL * KMAX), f32),
            pltpu.VMEM((C, NP_LOCAL * KMAX), bf16),
            pltpu.VMEM((PATCH, NP_LOCAL * KMAX), f32),
            pltpu.VMEM((C, NP_LOCAL * KMAX), bf16),
            pltpu.VMEM((384, NP_LOCAL * KMAX), bf16),
            pltpu.SemaphoreType.DMA((6,)),
            pltpu.SemaphoreType.DMA((6,)),
            pltpu.SemaphoreType.DMA((16,)),
        ],
        compiler_params=pltpu.CompilerParams(
            collective_id=0, has_side_effects=True
        ),
        name="cycle",
    )(facets, taper, *tables(), kernel[None], observed, patch_pos, counts, vis_u, vis_v)
    return residual, returned.reshape(2, C, 1, C)


def solution(mesh):
    both = ("role", "grp")
    return jax.shard_map(
        local,
        mesh=mesh,
        in_specs=(
            P("role", None, ("grp", "rep"), None),
            P("role", None),
            P(),
            P(None, both, "rep", None),
            P(both, "rep"),
            P(both, "rep"),
            P(both, "rep", None),
            P(both, "rep", None),
        ),
        out_specs=(P(None, both, "rep", None), P(None, None, ("grp", "rep"), None)),
        check_vma=False,
    )
```

```python
import math

import jax
import jax.numpy as jnp
import numpy as np
from jax import lax
from jax.experimental import pallas as pl
from jax.experimental.pallas import tpu as pltpu
from jax.sharding import PartitionSpec as P

F = 4096
C = 128
PATCH = 32
KW = 8
NP_LOCAL = 4
KMAX = 512
ROLES = 4
GRPS = 32
REPS = 4
NEAR = ROLES * REPS
FAR = 13
MESH = pl.DeviceIdType.MESH
bf16 = jnp.bfloat16
f32 = jnp.float32


def row_order():
    place = np.arange(C)
    return 4 * (place % GRPS) + place // GRPS


def tables():
    turn = 2.0 * math.pi
    row = row_order()
    cell = np.arange(128)
    block = np.arange(32)
    angle = turn * ((cell[:, None] * row[None, :]) % F) / F
    near = np.concatenate([np.cos(angle), -np.sin(angle)], axis=1)
    angle = turn * ((block[:, None] * row[None, :]) % 32) / 32
    far = np.concatenate([np.cos(angle), -np.sin(angle)], axis=1) / math.sqrt(F)
    angle = turn * ((cell[:, None] * block[None, :]) % 32) / 32
    cos, sin = np.cos(angle), np.sin(angle)
    first = np.block([[cos, sin], [-sin, cos]])
    angle = turn * ((cell[:, None] * cell[None, :]) % F) / F
    twist = np.concatenate([np.cos(angle), np.sin(angle)], axis=1)
    angle = turn * ((cell[:, None] * cell[None, :]) % 128) / 128
    cos, sin = np.cos(angle) / math.sqrt(F), np.sin(angle) / math.sqrt(F)
    second = np.stack([np.concatenate([cos, sin], 1), np.concatenate([-sin, cos], 1)], axis=1)
    second = second.reshape(ROLES, GRPS, 2, 256).transpose(1, 0, 2, 3).reshape(GRPS, 8, 256)
    return (
        jnp.asarray(near, bf16),
        jnp.asarray(far, f32),
        jnp.asarray(first, bf16),
        jnp.asarray(twist, f32),
        jnp.asarray(second, bf16),
    )


def mm(left, right):
    return lax.dot_general(left, right, (((1,), (0,)), ((), ())), preferred_element_type=f32)


def mm_t(left, right):
    return lax.dot_general(left, right, (((1,), (1,)), ((), ())), preferred_element_type=f32)


def body(
    facets_far, taper_far, near_far, far_far, first_far, twist_far, second_far,
    taps_far, observed_far, patch_pos_far, counts_far, vis_u_far, vis_v_far,
    residual, returned,
    facets, taper, near, far, first, twist, second,
    taps, observed, patch_pos, counts, vis_u, vis_v,
    x_out, x_in, q_out, q_in, q_all, u_all, u_out, s_in,
    y_out, y_in, z_all, z_out, z_in,
    ku, ku_low, kv, kv_wide, weights,
    sent, got, loaded,
):
    role, grp, rep = lax.axis_index("role"), lax.axis_index("grp"), lax.axis_index("rep")

    def near_peer(i):
        return (lax.rem(role + i // REPS, ROLES), grp, lax.rem(rep + i % REPS, REPS))

    def grp_peer(i):
        return lax.rem(grp + i, GRPS)

    inputs = [
        (taper_far, taper), (near_far, near), (far_far, far),
        (first_far, first), (twist_far, twist), (second_far, second),
        (taps_far, taps), (observed_far, observed), (patch_pos_far, patch_pos),
        (counts_far, counts), (vis_u_far, vis_u), (vis_v_far, vis_v),
    ]
    loads = []
    for k in range(4):
        part = pl.ds(1024 * k, 1024)
        loads.append((facets_far.at[0, :, :, part], facets.at[:, :, part]))
    loads = [
        pltpu.make_async_copy(src, dst, loaded.at[k]) for k, (src, dst) in enumerate(loads + inputs)
    ]
    for load in loads[4:7] + loads[:4] + loads[7:]:
        load.start()

    barrier = pltpu.get_barrier_semaphore()

    def greet_near(i, _):
        pl.semaphore_signal(barrier, inc=1, device_id=near_peer(i), device_id_type=MESH)
        return 0

    def greet_grp(i, _):
        pl.semaphore_signal(barrier, inc=1, device_id=(role, grp_peer(i), rep), device_id_type=MESH)
        return 0

    lax.fori_loop(1, GRPS, greet_grp, 0)
    lax.fori_loop(1, NEAR, greet_near, 0)

    def push(src, dst, phase, device):
        pltpu.make_async_remote_copy(
            src_ref=src, dst_ref=dst, send_sem=sent.at[phase], recv_sem=got.at[phase],
            device_id=device, device_id_type=MESH,
        ).start()

    def keep(src, dst, phase):
        pltpu.make_async_copy(src, dst, got.at[phase]).start()

    def arrive(buffer, phase):
        pltpu.make_async_copy(buffer, buffer, got.at[phase]).wait()

    def drain(buffer, count, phase):
        part = buffer.at[pl.ds(0, count)]
        pltpu.make_async_copy(part, part, sent.at[phase]).wait()

    for load in loads[4:7]:
        load.wait()
    table = near[...]
    part_re = jnp.zeros((32, C), f32)
    part_im = jnp.zeros((32, C), f32)
    for chunk in range(4):
        loads[chunk].wait()
        blocks = []
        for i in range(8 * chunk, 8 * chunk + 8):
            at = slice(128 * i, 128 * i + 128)
            blocks += [(facets[c, :, at].astype(f32) * taper[:, at]).astype(bf16) for c in range(2)]
        spectrum = mm(jnp.concatenate(blocks, axis=0), table)
        for k in range(8):
            i = 8 * chunk + k
            of_re = spectrum[64 * k : 64 * k + 32]
            of_im = spectrum[64 * k + 32 : 64 * k + 64]
            t_re = of_re[:, :C] - of_im[:, C:]
            t_im = of_re[:, C:] + of_im[:, :C]
            e_re = far[i : i + 1, :C]
            e_im = far[i : i + 1, C:]
            part_re = part_re + (t_re * e_re - t_im * e_im)
            part_im = part_im + (t_re * e_im + t_im * e_re)
    turned = jnp.concatenate([part_re, part_im, part_re, part_im], axis=0).T
    lane = lax.broadcasted_iota(jnp.int32, (1, 128), 1)
    own = taper[:, pl.ds(pl.multiple_of(grp * 128, 128), 128)]
    mine = jnp.zeros((1, 128), f32)
    for r in range(REPS):
        moved = own if r == 0 else pltpu.roll(own, 128 - 32 * r, 1)
        mine = mine + moved * jnp.where(rep == r, 1.0, 0.0)
    mine = jnp.where(lane < 32, mine, 0.0)
    mine = mine + pltpu.roll(mine, 32, 1)
    mine = mine + pltpu.roll(mine, 64, 1)
    turned = turned * mine
    for k in range(NEAR):
        x_out[k] = turned[8 * k : 8 * k + 8].astype(bf16)

    pl.semaphore_wait(barrier, GRPS + NEAR - 2)

    slot = role * REPS + rep

    def spread(out, into, phase):
        keep(out.at[slot], into.at[slot], phase)

        def send(i, _):
            device = near_peer(i)
            push(out.at[device[0] * REPS + device[2]], into.at[slot], phase, device)
            return 0

        lax.fori_loop(1, NEAR, send, 0)

    spread(x_out, x_in, 0)
    arrive(x_in, 0)
    cell_re = jnp.zeros((8, 128), f32)
    cell_im = jnp.zeros((8, 128), f32)
    for r in range(REPS):
        total = x_in[r].astype(f32)
        for k in range(1, ROLES):
            total = total + x_in[k * REPS + r].astype(f32)
        inside = (lane >= 32 * r) & (lane < 32 * r + 32)
        moved = pltpu.roll(total, 32, 1)
        cell_re = jnp.where(inside, total if r % 2 == 0 else moved, cell_re)
        cell_im = jnp.where(inside, moved if r % 2 == 0 else total, cell_im)
    q_out[0] = jnp.concatenate([cell_re, cell_im], axis=1).astype(bf16)
    keep(q_out.at[0], q_in.at[grp], 1)

    def send_cells(i, _):
        push(q_out.at[0], q_in.at[grp], 1, (role, grp_peer(i), rep))
        return 0

    lax.fori_loop(FAR, GRPS, send_cells, 0)
    lax.fori_loop(1, FAR, send_cells, 0)

    for load in loads[7:]:
        load.wait()
    sub = role * GRPS + grp
    place = lax.broadcasted_iota(jnp.int32, (PATCH, KMAX), 0)
    row_in_patch = 4 * (place % 8) + place // 8
    has_left = jnp.where(sub > 0, 1, 0)
    has_right = jnp.where(sub < ROLES * GRPS - 1, 1, 0)

    def block_of(p):
        position = jnp.broadcast_to(patch_pos[0:1, p : p + 1], (1, KMAX))
        row_block = (
            jnp.where(position >= 6, 1, 0)
            + jnp.where(position >= 12, 1, 0)
            + jnp.where(position >= 18, 1, 0)
        )
        return row_block, position - 6 * row_block

    tap = [jnp.broadcast_to(taps[0:1, t : t + 1], (PATCH, KMAX)) for t in range(KW)]
    for p in range(NP_LOCAL):
        cols = slice(KMAX * p, KMAX * p + KMAX)
        row_block, col_block = block_of(p)
        du = row_in_patch - vis_u[0, p : p + 1, :]
        dv = place - vis_v[0, p : p + 1, :]
        u32 = jnp.zeros((PATCH, KMAX), f32)
        v32 = jnp.zeros((PATCH, KMAX), f32)
        for t in range(KW):
            u32 = jnp.where(du == t, tap[t], u32)
            v32 = jnp.where(dv == t, tap[t], v32)
        kv[:, cols] = v32
        for r in range(REPS):
            rows = u32[8 * r : 8 * r + 8]
            for h in range(2):
                pair = jnp.concatenate(
                    [jnp.where(row_block == 2 * h + k, rows, 0.0) for k in range(2)], axis=0
                )
                at = slice(32 * r + 16 * h, 32 * r + 16 * h + 16)
                ku[at, cols] = pair
                ku_low[at, cols] = pair.astype(bf16)
        for u in range(4):
            chosen = jnp.where(col_block == u + 1, 1, 0)
            if u == 2:
                chosen = chosen + jnp.where(col_block == 0, 1, 0) * has_left
            if u == 1:
                chosen = chosen + jnp.where(col_block == 5, 1, 0) * has_right
            kv_wide[32 * u : 32 * u + 32, cols] = jnp.where(chosen > 0, v32, 0.0).astype(bf16)

    arrive(q_in, 1)
    for k in range(GRPS):
        arrived = q_in[k].astype(f32)
        q_all[8 * k : 8 * k + 8, :] = arrived[:, :128]
        q_all[8 * GRPS + 8 * k : 8 * GRPS + 8 * k + 8, :] = arrived[:, 128:]
    stacked = []
    for k in range(8):
        stacked.append(q_all[pl.ds(k, 2 * GRPS, stride=8), :].astype(bf16))
    mixed = mm(first[...], jnp.concatenate(stacked, axis=1))
    cos, sin = twist[:, :128], twist[:, 128:]
    both = []
    for k in range(8):
        mixed_re = mixed[:128, 128 * k : 128 * k + 128]
        mixed_im = mixed[128:, 128 * k : 128 * k + 128]
        pair = [mixed_re * cos + mixed_im * sin, mixed_im * cos - mixed_re * sin]
        both.append(jnp.concatenate(pair, axis=1).astype(bf16))
    waves = mm_t(second[grp], jnp.concatenate(both, axis=0))
    for k in range(8):
        u_all[8 * k : 8 * k + 8, :] = waves[:, 128 * k : 128 * k + 128]
    for k in range(ROLES):
        pair = [u_all[pl.ds(2 * k + c, 8, stride=8), :] for c in range(2)]
        u_out[k] = jnp.concatenate(pair, axis=1).astype(bf16)

    keep(u_out.at[role], s_in.at[slot], 2)

    def send_rows(i, _):
        device = near_peer(i)
        push(u_out.at[device[0]], s_in.at[slot], 2, device)
        return 0

    lax.fori_loop(1, NEAR, send_rows, 0)
    arrive(s_in, 2)

    rows = jnp.concatenate([s_in[k].astype(f32) for k in range(NEAR)], axis=0).astype(bf16)
    grid_cells = jnp.concatenate([rows[:, :128], rows[:, 128:]], axis=0)
    slots = lax.broadcasted_iota(jnp.int32, (1, KMAX), 1)
    for p in range(NP_LOCAL):
        cols = slice(KMAX * p, KMAX * p + KMAX)
        _, col_block = block_of(p)
        live = slots < jnp.broadcast_to(counts[0:1, p : p + 1], (1, KMAX))
        along = mm(grid_cells, kv_wide[:, cols])
        ku_p = ku[:, cols]
        kv_p = kv[:, cols]
        for c in range(2):
            predicted = jnp.sum(along[128 * c : 128 * c + 128] * ku_p, axis=0, keepdims=True)
            left_over = jnp.where(live, observed[c, 0, p : p + 1, :] - predicted, 0.0)
            residual[c, 0, p : p + 1, :] = left_over
            weighted = kv_p * left_over
            for u in range(4):
                at = slice(128 * c + 32 * u, 128 * c + 32 * u + 32)
                weights[at, cols] = jnp.where(col_block == u + 1, weighted, 0.0).astype(bf16)
            at = slice(256 + 64 * c, 256 + 64 * c + 32)
            weights[at, cols] = jnp.where(col_block == 0, weighted, 0.0).astype(bf16)
            at = slice(288 + 64 * c, 288 + 64 * c + 32)
            weights[at, cols] = jnp.where(col_block == 5, weighted, 0.0).astype(bf16)
    gridded = mm_t(ku_low[...], weights[...])
    for r in range(REPS):
        y_out[r] = gridded[32 * r : 32 * r + 32].astype(bf16)

    keep(y_out.at[rep], y_in.at[rep], 3)

    def send_gridded(i, _):
        to = lax.rem(rep + i, REPS)
        push(y_out.at[to], y_in.at[rep], 3, (role, grp, to))
        return 0

    lax.fori_loop(1, REPS, send_gridded, 0)
    arrive(y_in, 3)
    total = y_in[0].astype(f32)
    for r in range(1, REPS):
        total = total + y_in[r].astype(f32)
    z_all[pl.ds(3, GRPS, stride=4), :] = jnp.zeros((GRPS, 128), f32)
    for k in range(3):
        z_all[pl.ds(k, GRPS, stride=4), :] = total[:, 128 * k : 128 * k + 128]
    for k in range(GRPS):
        z_out[k] = z_all[4 * k : 4 * k + 4, :].astype(bf16)
    keep(z_out.at[grp], z_in.at[sub], 4)

    def send_owner(i, _):
        to = grp_peer(i)
        for k in range(ROLES):
            push(z_out.at[to], z_in.at[sub], 4, (lax.rem(role + k, ROLES), to, rep))
        return 0

    lax.fori_loop(FAR, GRPS, send_owner, 0)
    lax.fori_loop(1, FAR, send_owner, 0)
    for k in range(1, ROLES):
        push(z_out.at[grp], z_in.at[sub], 4, (lax.rem(role + k, ROLES), grp, rep))
    arrive(z_in, 4)

    for k in range(C):
        z_all[4 * k : 4 * k + 4, :] = z_in[k].astype(f32)
    owned = [z_all[pl.ds(k, C, stride=4), :] for k in range(3)]
    edges = owned[2]
    column = lax.broadcasted_iota(jnp.int32, (C, 128), 1)
    subgrid = lax.broadcasted_iota(jnp.int32, (C, 128), 0)
    for c in range(2):
        side = pltpu.roll(edges, 96 if c == 0 else 32, 1)
        from_left = jnp.where((column < 32) & (subgrid > 0), pltpu.roll(side, 1, 0), 0.0)
        from_right = jnp.where((column >= 96) & (subgrid < C - 1), pltpu.roll(side, C - 1, 0), 0.0)
        returned[c] = (owned[c] + from_left + from_right).astype(bf16)

    drain(x_in, NEAR - 1, 0)
    drain(q_in, GRPS - 1, 1)
    drain(s_in, NEAR - 1, 2)
    drain(y_in, REPS - 1, 3)
    drain(z_in, C - 1, 4)


def local(facets, taper, kernel, observed, patch_pos, counts, vis_u, vis_v):
    vmem = pl.BlockSpec(memory_space=pltpu.VMEM)
    hbm = pl.BlockSpec(memory_space=pltpu.HBM)
    residual, returned = pl.pallas_call(
        body,
        out_shape=(
            pltpu.VMEM((2, 1, NP_LOCAL, KMAX), f32),
            pltpu.VMEM((2, C, C), bf16),
        ),
        in_specs=[hbm] * 13,
        out_specs=(vmem, vmem),
        scratch_shapes=[
            pltpu.VMEM((2, 32, F), bf16),
            pltpu.VMEM((1, F), f32),
            pltpu.VMEM((128, 256), bf16),
            pltpu.VMEM((32, 256), f32),
            pltpu.VMEM((256, 64), bf16),
            pltpu.VMEM((128, 256), f32),
            pltpu.VMEM((GRPS, 8, 256), bf16),
            pltpu.VMEM((1, KW), f32),
            pltpu.VMEM((2, 1, NP_LOCAL, KMAX), f32),
            pltpu.VMEM((1, NP_LOCAL), jnp.int32),
            pltpu.VMEM((1, NP_LOCAL), jnp.int32),
            pltpu.VMEM((1, NP_LOCAL, KMAX), jnp.int32),
            pltpu.VMEM((1, NP_LOCAL, KMAX), jnp.int32),
            pltpu.VMEM((NEAR, 8, 128), bf16),
            pltpu.VMEM((NEAR, 8, 128), bf16),
            pltpu.VMEM((1, 8, 256), bf16),
            pltpu.VMEM((GRPS, 8, 256), bf16),
            pltpu.VMEM((16 * GRPS, 128), f32),
            pltpu.VMEM((64, 128), f32),
            pltpu.VMEM((ROLES, 8, 256), bf16),
            pltpu.VMEM((NEAR, 8, 256), bf16),
            pltpu.VMEM((REPS, 32, 384), bf16),
            pltpu.VMEM((REPS, 32, 384), bf16),
            pltpu.VMEM((4 * C, 128), f32),
            pltpu.VMEM((GRPS, 4, 128), bf16),
            pltpu.VMEM((C, 4, 128), bf16),
            pltpu.VMEM((C, NP_LOCAL * KMAX), f32),
            pltpu.VMEM((C, NP_LOCAL * KMAX), bf16),
            pltpu.VMEM((PATCH, NP_LOCAL * KMAX), f32),
            pltpu.VMEM((C, NP_LOCAL * KMAX), bf16),
            pltpu.VMEM((384, NP_LOCAL * KMAX), bf16),
            pltpu.SemaphoreType.DMA((5,)),
            pltpu.SemaphoreType.DMA((5,)),
            pltpu.SemaphoreType.DMA((16,)),
        ],
        compiler_params=pltpu.CompilerParams(
            collective_id=0, has_side_effects=True
        ),
        name="cycle",
    )(facets, taper, *tables(), kernel[None], observed, patch_pos, counts, vis_u, vis_v)
    return residual, returned.reshape(2, C, 1, C)


def solution(mesh):
    both = ("role", "grp")
    return jax.shard_map(
        local,
        mesh=mesh,
        in_specs=(
            P("role", None, ("grp", "rep"), None),
            P("role", None),
            P(),
            P(None, both, "rep", None),
            P(both, "rep"),
            P(both, "rep"),
            P(both, "rep", None),
            P(both, "rep", None),
        ),
        out_specs=(P(None, both, "rep", None), P(None, None, ("grp", "rep"), None)),
        check_vma=False,
    )
```

```python
import math

import jax
import jax.numpy as jnp
import numpy as np
from jax import lax
from jax.experimental import pallas as pl
from jax.experimental.pallas import tpu as pltpu
from jax.sharding import PartitionSpec as P

F = 4096
C = 128
PATCH = 32
KW = 8
NP_LOCAL = 4
KMAX = 512
ROLES = 4
GRPS = 32
REPS = 4
NEAR = ROLES * REPS
MESH = pl.DeviceIdType.MESH
bf16 = jnp.bfloat16
f32 = jnp.float32


def row_order():
    place = np.arange(C)
    return 4 * (place % GRPS) + place // GRPS


def tables():
    turn = 2.0 * math.pi
    row = row_order()
    cell = np.arange(128)
    block = np.arange(32)
    angle = turn * ((cell[:, None] * row[None, :]) % F) / F
    near = np.concatenate([np.cos(angle), -np.sin(angle)], axis=1)
    angle = turn * ((block[:, None] * row[None, :]) % 32) / 32
    far = np.concatenate([np.cos(angle), -np.sin(angle)], axis=1) / math.sqrt(F)
    angle = turn * ((cell[:, None] * block[None, :]) % 32) / 32
    cos, sin = np.cos(angle), np.sin(angle)
    first = np.block([[cos, sin], [-sin, cos]])
    angle = turn * ((cell[:, None] * cell[None, :]) % F) / F
    twist = np.concatenate([np.cos(angle), np.sin(angle)], axis=1)
    angle = turn * ((cell[:, None] * cell[None, :]) % 128) / 128
    cos, sin = np.cos(angle) / math.sqrt(F), np.sin(angle) / math.sqrt(F)
    second = np.stack([np.concatenate([cos, sin], 1), np.concatenate([-sin, cos], 1)], axis=1)
    second = second.reshape(ROLES, GRPS, 2, 256).transpose(1, 0, 2, 3).reshape(GRPS, 8, 256)
    return (
        jnp.asarray(near, bf16),
        jnp.asarray(far, f32),
        jnp.asarray(first, bf16),
        jnp.asarray(twist, f32),
        jnp.asarray(second, bf16),
    )


def mm(left, right):
    return lax.dot_general(left, right, (((1,), (0,)), ((), ())), preferred_element_type=f32)


def mm_t(left, right):
    return lax.dot_general(left, right, (((1,), (1,)), ((), ())), preferred_element_type=f32)


def body(
    facets_far, taper_far, near_far, far_far, first_far, twist_far, second_far,
    taps_far, observed_far, patch_pos_far, counts_far, vis_u_far, vis_v_far,
    residual, returned,
    facets, taper, near, far, first, twist, second,
    taps, observed, patch_pos, counts, vis_u, vis_v,
    x_out, x_in, q_out, q_in, q_all, u_all, u_out, s_in,
    z_all, z_out, z_in, s_all, left,
    ku, kv, kv_wide,
    sent, got, loaded,
):
    role, grp, rep = lax.axis_index("role"), lax.axis_index("grp"), lax.axis_index("rep")

    def near_peer(i):
        return (lax.rem(role + i // REPS, ROLES), grp, lax.rem(rep + i % REPS, REPS))

    def grp_peer(i):
        return lax.rem(grp + i, GRPS)

    def for_grps(send):
        for dz in (2, 1, 3):
            base = lax.rem(grp // 8 + dz, 4) * 8

            def step(i, _, base=base):
                send(base + lax.rem(grp + i, 8))
                return 0

            lax.fori_loop(3, 11, step, 0)

        def last(i, _):
            send((grp // 8) * 8 + lax.rem(grp + 1 + lax.rem(i, 7), 8))
            return 0

        lax.fori_loop(2, 9, last, 0)

    inputs = [
        (taper_far, taper), (near_far, near), (far_far, far),
        (first_far, first), (twist_far, twist), (second_far, second), (taps_far, taps),
        (observed_far, observed.at[rep]), (patch_pos_far, patch_pos.at[rep]),
        (counts_far, counts.at[rep]), (vis_u_far, vis_u.at[rep]), (vis_v_far, vis_v.at[rep]),
    ]
    loads = []
    for k in range(4):
        part = pl.ds(1024 * k, 1024)
        loads.append((facets_far.at[0, :, :, part], facets.at[:, :, part]))
    loads = [
        pltpu.make_async_copy(src, dst, loaded.at[k]) for k, (src, dst) in enumerate(loads + inputs)
    ]
    for load in loads[4:7] + loads[:4] + loads[7:]:
        load.start()

    barrier = pltpu.get_barrier_semaphore()

    def greet_near(i, _):
        pl.semaphore_signal(barrier, inc=1, device_id=near_peer(i), device_id_type=MESH)
        return 0

    def greet_grp(i, _):
        pl.semaphore_signal(barrier, inc=1, device_id=(role, grp_peer(i), rep), device_id_type=MESH)
        return 0

    lax.fori_loop(1, GRPS, greet_grp, 0)
    lax.fori_loop(1, NEAR, greet_near, 0)

    def push(src, dst, phase, device):
        pltpu.make_async_remote_copy(
            src_ref=src, dst_ref=dst, send_sem=sent.at[phase], recv_sem=got.at[phase],
            device_id=device, device_id_type=MESH,
        ).start()

    def keep(src, dst, phase):
        pltpu.make_async_copy(src, dst, got.at[phase]).start()

    def arrive(buffer, phase):
        pltpu.make_async_copy(buffer, buffer, got.at[phase]).wait()

    def drain(buffer, count, phase):
        part = buffer.at[pl.ds(0, count)]
        pltpu.make_async_copy(part, part, sent.at[phase]).wait()

    for load in loads[4:7]:
        load.wait()
    table = near[...]
    part_re = jnp.zeros((32, C), f32)
    part_im = jnp.zeros((32, C), f32)
    for chunk in range(4):
        loads[chunk].wait()
        blocks = []
        for i in range(8 * chunk, 8 * chunk + 8):
            at = slice(128 * i, 128 * i + 128)
            blocks += [(facets[c, :, at].astype(f32) * taper[:, at]).astype(bf16) for c in range(2)]
        spectrum = mm(jnp.concatenate(blocks, axis=0), table)
        for k in range(8):
            i = 8 * chunk + k
            of_re = spectrum[64 * k : 64 * k + 32]
            of_im = spectrum[64 * k + 32 : 64 * k + 64]
            t_re = of_re[:, :C] - of_im[:, C:]
            t_im = of_re[:, C:] + of_im[:, :C]
            e_re = far[i : i + 1, :C]
            e_im = far[i : i + 1, C:]
            part_re = part_re + (t_re * e_re - t_im * e_im)
            part_im = part_im + (t_re * e_im + t_im * e_re)
    turned = jnp.concatenate([part_re, part_im, part_re, part_im], axis=0).T
    lane = lax.broadcasted_iota(jnp.int32, (1, 128), 1)
    own = taper[:, pl.ds(pl.multiple_of(grp * 128, 128), 128)]
    mine = jnp.zeros((1, 128), f32)
    for r in range(REPS):
        moved = own if r == 0 else pltpu.roll(own, 128 - 32 * r, 1)
        mine = mine + moved * jnp.where(rep == r, 1.0, 0.0)
    mine = jnp.where(lane < 32, mine, 0.0)
    mine = mine + pltpu.roll(mine, 32, 1)
    mine = mine + pltpu.roll(mine, 64, 1)
    turned = turned * mine
    for k in range(NEAR):
        x_out[k] = turned[8 * k : 8 * k + 8].astype(bf16)

    pl.semaphore_wait(barrier, GRPS + NEAR - 2)

    slot = role * REPS + rep

    def spread(out, into, phase):
        keep(out.at[slot], into.at[slot], phase)

        def send(i, _):
            device = near_peer(i)
            push(out.at[device[0] * REPS + device[2]], into.at[slot], phase, device)
            return 0

        lax.fori_loop(1, NEAR, send, 0)

    spread(x_out, x_in, 0)
    arrive(x_in, 0)
    cell_re = jnp.zeros((8, 128), f32)
    cell_im = jnp.zeros((8, 128), f32)
    for r in range(REPS):
        total = x_in[r].astype(f32)
        for k in range(1, ROLES):
            total = total + x_in[k * REPS + r].astype(f32)
        inside = (lane >= 32 * r) & (lane < 32 * r + 32)
        moved = pltpu.roll(total, 32, 1)
        cell_re = jnp.where(inside, total if r % 2 == 0 else moved, cell_re)
        cell_im = jnp.where(inside, moved if r % 2 == 0 else total, cell_im)
    q_out[0] = jnp.concatenate([cell_re, cell_im], axis=1).astype(bf16)
    keep(q_out.at[0], q_in.at[grp], 1)

    def send_cells(to):
        push(q_out.at[0], q_in.at[grp], 1, (role, to, rep))

    for_grps(send_cells)

    for load in loads[7:]:
        load.wait()
    shared = (observed, patch_pos, counts, vis_u, vis_v)
    for k, held in enumerate(shared):

        def send_held(i, _, held=held, k=k):
            push(held.at[rep], held.at[rep], 4 + k, (role, grp, lax.rem(rep + i, REPS)))
            return 0

        lax.fori_loop(1, REPS, send_held, 0)
    for k, held in enumerate(shared):
        part = held.at[pl.ds(0, REPS - 1)]
        pltpu.make_async_copy(part, part, got.at[4 + k]).wait()

    sub = role * GRPS + grp
    place = lax.broadcasted_iota(jnp.int32, (PATCH, KMAX), 0)
    row_in_patch = 4 * (place % 8) + place // 8
    has_left = jnp.where(sub > 0, 1, 0)
    has_right = jnp.where(sub < ROLES * GRPS - 1, 1, 0)

    def block_of(k, p, width):
        position = jnp.broadcast_to(patch_pos[k, 0:1, p : p + 1], (1, width))
        row_block = (
            jnp.where(position >= 6, 1, 0)
            + jnp.where(position >= 12, 1, 0)
            + jnp.where(position >= 18, 1, 0)
        )
        return row_block, position - 6 * row_block

    patches = [(k, p) for k in range(REPS) for p in range(NP_LOCAL)]
    tap = [jnp.broadcast_to(taps[0:1, t : t + 1], (PATCH, KMAX)) for t in range(KW)]
    for k, p in patches:
        cols = slice(KMAX * (NP_LOCAL * k + p), KMAX * (NP_LOCAL * k + p + 1))
        _, col_block = block_of(k, p, KMAX)
        du = row_in_patch - vis_u[k, 0, p : p + 1, :]
        dv = place - vis_v[k, 0, p : p + 1, :]
        u32 = jnp.zeros((PATCH, KMAX), f32)
        v32 = jnp.zeros((PATCH, KMAX), f32)
        for t in range(KW):
            u32 = jnp.where(du == t, tap[t], u32)
            v32 = jnp.where(dv == t, tap[t], v32)
        ku[:, cols] = u32
        kv[:, cols] = v32
        for u in range(4):
            chosen = jnp.where(col_block == u + 1, 1, 0)
            if u == 2:
                chosen = chosen + jnp.where(col_block == 0, 1, 0) * has_left
            if u == 1:
                chosen = chosen + jnp.where(col_block == 5, 1, 0) * has_right
            kv_wide[32 * u : 32 * u + 32, cols] = jnp.where(chosen > 0, v32, 0.0).astype(bf16)

    arrive(q_in, 1)
    for k in range(GRPS):
        arrived = q_in[k].astype(f32)
        q_all[8 * k : 8 * k + 8, :] = arrived[:, :128]
        q_all[8 * GRPS + 8 * k : 8 * GRPS + 8 * k + 8, :] = arrived[:, 128:]
    stacked = []
    for k in range(8):
        stacked.append(q_all[pl.ds(k, 2 * GRPS, stride=8), :].astype(bf16))
    mixed = mm(first[...], jnp.concatenate(stacked, axis=1))
    cos, sin = twist[:, :128], twist[:, 128:]
    both = []
    for k in range(8):
        mixed_re = mixed[:128, 128 * k : 128 * k + 128]
        mixed_im = mixed[128:, 128 * k : 128 * k + 128]
        pair = [mixed_re * cos + mixed_im * sin, mixed_im * cos - mixed_re * sin]
        both.append(jnp.concatenate(pair, axis=1).astype(bf16))
    waves = mm_t(second[grp], jnp.concatenate(both, axis=0))
    for k in range(8):
        u_all[8 * k : 8 * k + 8, :] = waves[:, 128 * k : 128 * k + 128]
    for k in range(ROLES):
        pair = [u_all[pl.ds(2 * k + c, 8, stride=8), :] for c in range(2)]
        u_out[k] = jnp.concatenate(pair, axis=1).astype(bf16)

    keep(u_out.at[role], s_in.at[slot], 2)

    def send_rows(i, _):
        device = near_peer(i)
        push(u_out.at[device[0]], s_in.at[slot], 2, device)
        return 0

    lax.fori_loop(1, NEAR, send_rows, 0)
    arrive(s_in, 2)

    for k in range(NEAR):
        arrived = s_in[k].astype(f32)
        for c in range(2):
            s_all[128 * c + 8 * k : 128 * c + 8 * k + 8, :] = arrived[:, 128 * c : 128 * c + 128]
    slots = lax.broadcasted_iota(jnp.int32, (1, KMAX), 1)
    total = [[jnp.zeros((8, 128), f32) for _ in range(4)] for _ in range(3)]
    for k, p in patches:
        cols = slice(KMAX * (NP_LOCAL * k + p), KMAX * (NP_LOCAL * k + p + 1))
        row_block, col_block = block_of(k, p, 128)
        rows = []
        for m in range(8):
            block = s_all[32 * m : 32 * m + 8, :]
            for h in range(1, 4):
                at = slice(32 * m + 8 * h, 32 * m + 8 * h + 8)
                block = jnp.where(row_block == h, s_all[at, :], block)
            rows.append(block)
        along = mm(jnp.concatenate(rows, axis=0).astype(bf16), kv_wide[:, cols])
        live = slots < jnp.broadcast_to(counts[k, 0:1, p : p + 1], (1, KMAX))
        ku_p = ku[:, cols]
        kv_p = kv[:, cols]
        weighted = []
        for c in range(2):
            predicted = jnp.sum(along[32 * c : 32 * c + 32] * ku_p, axis=0, keepdims=True)
            left_over = jnp.where(live, observed[k, c, 0, p : p + 1, :] - predicted, 0.0)
            left[k, c, 0, p : p + 1, :] = left_over
            weighted.append((kv_p * left_over).astype(bf16))
        mine_u = ku[pl.ds(pl.multiple_of(8 * rep, 8), 8), cols].astype(bf16)
        both = mm_t(mine_u, jnp.concatenate(weighted + weighted, axis=0))
        turned = pltpu.roll(both, 32, 1)
        even = (lane // 32) % 2 == 0
        pieces = (
            (jnp.where(even, both, turned), lane // 32 == col_block - 1),
            (jnp.where(even, turned, both), lane // 32 == col_block - 1),
            (
                jnp.where((lane < 32) | (lane >= 96), both, turned),
                jnp.where(even, 0, 5) == col_block,
            ),
        )
        for j, (piece, inside) in enumerate(pieces):
            for h in range(4):
                here = jnp.where(row_block == h, 1, 0) * jnp.where(inside, 1, 0)
                total[j][h] = total[j][h] + jnp.where(here > 0, piece, 0.0)

    z_all[pl.ds(3, GRPS, stride=4), :] = jnp.zeros((GRPS, 128), f32)
    for k in range(3):
        z_all[pl.ds(k, GRPS, stride=4), :] = jnp.concatenate(total[k], axis=0)
    for k in range(GRPS):
        z_out[k] = z_all[4 * k : 4 * k + 4, :].astype(bf16)
    keep(z_out.at[grp], z_in.at[sub], 3)

    def send_owner(to):
        for k in range(ROLES):
            push(z_out.at[to], z_in.at[sub], 3, (lax.rem(role + k, ROLES), to, rep))

    for_grps(send_owner)
    for k in range(1, ROLES):
        push(z_out.at[grp], z_in.at[sub], 3, (lax.rem(role + k, ROLES), grp, rep))
    residual[...] = left[rep]
    arrive(z_in, 3)

    for k in range(C):
        z_all[4 * k : 4 * k + 4, :] = z_in[k].astype(f32)
    owned = [z_all[pl.ds(k, C, stride=4), :] for k in range(3)]
    edges = owned[2]
    column = lax.broadcasted_iota(jnp.int32, (C, 128), 1)
    subgrid = lax.broadcasted_iota(jnp.int32, (C, 128), 0)
    for c in range(2):
        side = pltpu.roll(edges, 96 if c == 0 else 32, 1)
        from_left = jnp.where((column < 32) & (subgrid > 0), pltpu.roll(side, 1, 0), 0.0)
        from_right = jnp.where((column >= 96) & (subgrid < C - 1), pltpu.roll(side, C - 1, 0), 0.0)
        returned[c] = (owned[c] + from_left + from_right).astype(bf16)

    drain(x_in, NEAR - 1, 0)
    drain(q_in, GRPS - 1, 1)
    drain(s_in, NEAR - 1, 2)
    drain(z_in, C - 1, 3)
    for k, held in enumerate(shared):
        drain(held, REPS - 1, 4 + k)


def flush(residual, returned, residual_out, returned_out, done):
    copies = [
        pltpu.make_async_copy(returned, returned_out, done.at[0]),
        pltpu.make_async_copy(residual, residual_out, done.at[1]),
    ]
    for copy in copies:
        copy.start()
    for copy in copies:
        copy.wait()


def local(facets, taper, kernel, observed, patch_pos, counts, vis_u, vis_v):
    vmem = pl.BlockSpec(memory_space=pltpu.VMEM)
    hbm = pl.BlockSpec(memory_space=pltpu.HBM)
    residual, returned = pl.pallas_call(
        body,
        out_shape=(
            pltpu.VMEM((2, 1, NP_LOCAL, KMAX), f32),
            pltpu.VMEM((2, C, C), bf16),
        ),
        in_specs=[hbm] * 13,
        out_specs=(vmem, vmem),
        scratch_shapes=[
            pltpu.VMEM((2, 32, F), bf16),
            pltpu.VMEM((1, F), f32),
            pltpu.VMEM((128, 256), bf16),
            pltpu.VMEM((32, 256), f32),
            pltpu.VMEM((256, 64), bf16),
            pltpu.VMEM((128, 256), f32),
            pltpu.VMEM((GRPS, 8, 256), bf16),
            pltpu.VMEM((1, KW), f32),
            pltpu.VMEM((REPS, 2, 1, NP_LOCAL, KMAX), f32),
            pltpu.VMEM((REPS, 1, NP_LOCAL), jnp.int32),
            pltpu.VMEM((REPS, 1, NP_LOCAL), jnp.int32),
            pltpu.VMEM((REPS, 1, NP_LOCAL, KMAX), jnp.int32),
            pltpu.VMEM((REPS, 1, NP_LOCAL, KMAX), jnp.int32),
            pltpu.VMEM((NEAR, 8, 128), bf16),
            pltpu.VMEM((NEAR, 8, 128), bf16),
            pltpu.VMEM((1, 8, 256), bf16),
            pltpu.VMEM((GRPS, 8, 256), bf16),
            pltpu.VMEM((16 * GRPS, 128), f32),
            pltpu.VMEM((64, 128), f32),
            pltpu.VMEM((ROLES, 8, 256), bf16),
            pltpu.VMEM((NEAR, 8, 256), bf16),
            pltpu.VMEM((4 * C, 128), f32),
            pltpu.VMEM((GRPS, 4, 128), bf16),
            pltpu.VMEM((C, 4, 128), bf16),
            pltpu.VMEM((2 * C, 128), f32),
            pltpu.VMEM((REPS, 2, 1, NP_LOCAL, KMAX), f32),
            pltpu.VMEM((PATCH, REPS * NP_LOCAL * KMAX), f32),
            pltpu.VMEM((PATCH, REPS * NP_LOCAL * KMAX), f32),
            pltpu.VMEM((C, REPS * NP_LOCAL * KMAX), bf16),
            pltpu.SemaphoreType.DMA((9,)),
            pltpu.SemaphoreType.DMA((9,)),
            pltpu.SemaphoreType.DMA((16,)),
        ],
        compiler_params=pltpu.CompilerParams(
            collective_id=0, has_side_effects=True
        ),
        name="cycle",
    )(facets, taper, *tables(), kernel[None], observed, patch_pos, counts, vis_u, vis_v)
    anywhere = pl.BlockSpec(memory_space=pl.ANY)
    residual, returned = pl.pallas_call(
        flush,
        out_shape=(
            jax.ShapeDtypeStruct((2, 1, NP_LOCAL, KMAX), f32),
            jax.ShapeDtypeStruct((2, C, C), bf16),
        ),
        in_specs=[vmem, vmem],
        out_specs=(anywhere, anywhere),
        scratch_shapes=[pltpu.SemaphoreType.DMA((2,))],
        compiler_params=pltpu.CompilerParams(vmem_limit_bytes=1 << 20),
        name="flush",
    )(residual, returned)
    return residual, returned.reshape(2, C, 1, C)


def solution(mesh):
    both = ("role", "grp")
    return jax.shard_map(
        local,
        mesh=mesh,
        in_specs=(
            P("role", None, ("grp", "rep"), None),
            P("role", None),
            P(),
            P(None, both, "rep", None),
            P(both, "rep"),
            P(both, "rep"),
            P(both, "rep", None),
            P(both, "rep", None),
        ),
        out_specs=(P(None, both, "rep", None), P(None, None, ("grp", "rep"), None)),
        check_vma=False,
    )
```

```python
import math

import jax
import jax.numpy as jnp
import numpy as np
from jax import lax
from jax.experimental import pallas as pl
from jax.experimental.pallas import tpu as pltpu
from jax.sharding import PartitionSpec as P

F = 4096
C = 128
PATCH = 32
KW = 8
NP_LOCAL = 4
KMAX = 512
ROLES = 4
GRPS = 32
REPS = 4
NEAR = ROLES * REPS
MESH = pl.DeviceIdType.MESH
bf16 = jnp.bfloat16
f32 = jnp.float32


def row_order():
    place = np.arange(C)
    return 4 * (place % GRPS) + place // GRPS


def tables():
    turn = 2.0 * math.pi
    row = row_order()
    cell = np.arange(128)
    block = np.arange(32)
    angle = turn * ((cell[:, None] * row[None, :]) % F) / F
    near = np.concatenate([np.cos(angle), -np.sin(angle)], axis=1)
    angle = turn * ((block[:, None] * row[None, :]) % 32) / 32
    far = np.concatenate([np.cos(angle), -np.sin(angle)], axis=1) / math.sqrt(F)
    angle = turn * ((cell[:, None] * block[None, :]) % 32) / 32
    cos, sin = np.cos(angle), np.sin(angle)
    first = np.block([[cos, sin], [-sin, cos]])
    angle = turn * ((cell[:, None] * cell[None, :]) % F) / F
    twist = np.concatenate([np.cos(angle), np.sin(angle)], axis=1)
    angle = turn * ((cell[:, None] * cell[None, :]) % 128) / 128
    cos, sin = np.cos(angle) / math.sqrt(F), np.sin(angle) / math.sqrt(F)
    second = np.stack([np.concatenate([cos, sin], 1), np.concatenate([-sin, cos], 1)], axis=1)
    second = second.reshape(ROLES, GRPS, 2, 256).transpose(1, 0, 2, 3).reshape(GRPS, 8, 256)
    return (
        jnp.asarray(near, bf16),
        jnp.asarray(far, f32),
        jnp.asarray(first, bf16),
        jnp.asarray(twist, f32),
        jnp.asarray(second, bf16),
    )


def mm(left, right):
    return lax.dot_general(left, right, (((1,), (0,)), ((), ())), preferred_element_type=f32)


def mm_t(left, right):
    return lax.dot_general(left, right, (((1,), (1,)), ((), ())), preferred_element_type=f32)


def body(
    facets_far, taper_far, near_far, far_far, first_far, twist_far, second_far,
    taps_far, observed_far, patch_pos_far, counts_far, vis_u_far, vis_v_far,
    residual, returned,
    facets, taper, near, far, first, twist, second,
    taps, observed, patch_pos, counts, vis_u, vis_v,
    x_out, x_in, q_out, q_in, q_all, u_all, u_out, s_in,
    z_all, z_out, z_in, s_all, left,
    ku, kv, kv_wide,
    sent, got, loaded,
):
    role, grp, rep = lax.axis_index("role"), lax.axis_index("grp"), lax.axis_index("rep")

    def near_peer(i):
        return (lax.rem(role + i // REPS, ROLES), grp, lax.rem(rep + i % REPS, REPS))

    def grp_peer(i):
        return lax.rem(grp + i, GRPS)

    def for_grps(send):
        for dz in (2, 1, 3):
            base = lax.rem(grp // 8 + dz, 4) * 8

            def step(i, _, base=base):
                send(base + lax.rem(grp + i, 8))
                return 0

            lax.fori_loop(3, 11, step, 0)

        def last(i, _):
            send((grp // 8) * 8 + lax.rem(grp + 1 + lax.rem(i, 7), 8))
            return 0

        lax.fori_loop(2, 9, last, 0)

    inputs = [
        (taper_far, taper), (near_far, near), (far_far, far),
        (first_far, first), (twist_far, twist), (second_far, second), (taps_far, taps),
        (observed_far, observed.at[rep]), (patch_pos_far, patch_pos.at[rep]),
        (counts_far, counts.at[rep]), (vis_u_far, vis_u.at[rep]), (vis_v_far, vis_v.at[rep]),
    ]
    loads = []
    for k in range(4):
        part = pl.ds(1024 * k, 1024)
        loads.append((facets_far.at[0, :, :, part], facets.at[:, :, part]))
    loads = [
        pltpu.make_async_copy(src, dst, loaded.at[k]) for k, (src, dst) in enumerate(loads + inputs)
    ]
    for load in loads[4:7] + loads[:4] + loads[7:]:
        load.start()

    barrier = pltpu.get_barrier_semaphore()

    def greet_near(i, _):
        pl.semaphore_signal(barrier, inc=1, device_id=near_peer(i), device_id_type=MESH)
        return 0

    def greet_grp(i, _):
        pl.semaphore_signal(barrier, inc=1, device_id=(role, grp_peer(i), rep), device_id_type=MESH)
        return 0

    lax.fori_loop(1, GRPS, greet_grp, 0)
    lax.fori_loop(1, NEAR, greet_near, 0)

    def push(src, dst, phase, device):
        pltpu.make_async_remote_copy(
            src_ref=src, dst_ref=dst, send_sem=sent.at[phase], recv_sem=got.at[phase],
            device_id=device, device_id_type=MESH,
        ).start()

    def keep(src, dst, phase):
        pltpu.make_async_copy(src, dst, got.at[phase]).start()

    def arrive(buffer, phase):
        pltpu.make_async_copy(buffer, buffer, got.at[phase]).wait()

    def drain(buffer, count, phase):
        part = buffer.at[pl.ds(0, count)]
        pltpu.make_async_copy(part, part, sent.at[phase]).wait()

    for load in loads[:7]:
        load.wait()
    table = near[...]
    part_re = jnp.zeros((32, C), f32)
    part_im = jnp.zeros((32, C), f32)
    for chunk in range(4):
        blocks = []
        for i in range(8 * chunk, 8 * chunk + 8):
            at = slice(128 * i, 128 * i + 128)
            blocks += [(facets[c, :, at].astype(f32) * taper[:, at]).astype(bf16) for c in range(2)]
        spectrum = mm(jnp.concatenate(blocks, axis=0), table)
        for k in range(8):
            i = 8 * chunk + k
            of_re = spectrum[64 * k : 64 * k + 32]
            of_im = spectrum[64 * k + 32 : 64 * k + 64]
            t_re = of_re[:, :C] - of_im[:, C:]
            t_im = of_re[:, C:] + of_im[:, :C]
            e_re = far[i : i + 1, :C]
            e_im = far[i : i + 1, C:]
            part_re = part_re + (t_re * e_re - t_im * e_im)
            part_im = part_im + (t_re * e_im + t_im * e_re)
    turned = jnp.concatenate([part_re, part_im, part_re, part_im], axis=0).T
    lane = lax.broadcasted_iota(jnp.int32, (1, 128), 1)
    own = taper[:, pl.ds(pl.multiple_of(grp * 128, 128), 128)]
    mine = jnp.zeros((1, 128), f32)
    for r in range(REPS):
        moved = own if r == 0 else pltpu.roll(own, 128 - 32 * r, 1)
        mine = mine + moved * jnp.where(rep == r, 1.0, 0.0)
    mine = jnp.where(lane < 32, mine, 0.0)
    mine = mine + pltpu.roll(mine, 32, 1)
    mine = mine + pltpu.roll(mine, 64, 1)
    turned = turned * mine
    for k in range(NEAR):
        x_out[k] = turned[8 * k : 8 * k + 8].astype(bf16)

    pl.semaphore_wait(barrier, GRPS + NEAR - 2)

    slot = role * REPS + rep

    def spread(out, into, phase):
        keep(out.at[slot], into.at[slot], phase)

        def send(i, _):
            device = near_peer(i)
            push(out.at[device[0] * REPS + device[2]], into.at[slot], phase, device)
            return 0

        lax.fori_loop(1, NEAR, send, 0)

    spread(x_out, x_in, 0)
    arrive(x_in, 0)
    cell_re = jnp.zeros((8, 128), f32)
    cell_im = jnp.zeros((8, 128), f32)
    for r in range(REPS):
        total = x_in[r].astype(f32)
        for k in range(1, ROLES):
            total = total + x_in[k * REPS + r].astype(f32)
        inside = (lane >= 32 * r) & (lane < 32 * r + 32)
        moved = pltpu.roll(total, 32, 1)
        cell_re = jnp.where(inside, total if r % 2 == 0 else moved, cell_re)
        cell_im = jnp.where(inside, moved if r % 2 == 0 else total, cell_im)
    q_out[0] = jnp.concatenate([cell_re, cell_im], axis=1).astype(bf16)
    keep(q_out.at[0], q_in.at[grp], 1)

    def send_cells(to):
        push(q_out.at[0], q_in.at[grp], 1, (role, to, rep))

    for_grps(send_cells)

    for load in loads[7:]:
        load.wait()
    shared = (observed, patch_pos, counts, vis_u, vis_v)
    for k, held in enumerate(shared):

        def send_held(i, _, held=held, k=k):
            push(held.at[rep], held.at[rep], 4 + k, (role, grp, lax.rem(rep + i, REPS)))
            return 0

        lax.fori_loop(1, REPS, send_held, 0)
    for k, held in enumerate(shared):
        part = held.at[pl.ds(0, REPS - 1)]
        pltpu.make_async_copy(part, part, got.at[4 + k]).wait()

    sub = role * GRPS + grp
    place = lax.broadcasted_iota(jnp.int32, (PATCH, KMAX), 0)
    row_in_patch = 4 * (place % 8) + place // 8
    has_left = jnp.where(sub > 0, 1, 0)
    has_right = jnp.where(sub < ROLES * GRPS - 1, 1, 0)

    def block_of(k, p, width):
        position = jnp.broadcast_to(patch_pos[k, 0:1, p : p + 1], (1, width))
        row_block = (
            jnp.where(position >= 6, 1, 0)
            + jnp.where(position >= 12, 1, 0)
            + jnp.where(position >= 18, 1, 0)
        )
        return row_block, position - 6 * row_block

    patches = [(k, p) for k in range(REPS) for p in range(NP_LOCAL)]
    tap = [jnp.broadcast_to(taps[0:1, t : t + 1], (PATCH, KMAX)) for t in range(KW)]
    for k, p in patches:
        cols = slice(KMAX * (NP_LOCAL * k + p), KMAX * (NP_LOCAL * k + p + 1))
        _, col_block = block_of(k, p, KMAX)
        du = row_in_patch - vis_u[k, 0, p : p + 1, :]
        dv = place - vis_v[k, 0, p : p + 1, :]
        u32 = jnp.zeros((PATCH, KMAX), f32)
        v32 = jnp.zeros((PATCH, KMAX), f32)
        for t in range(KW):
            u32 = jnp.where(du == t, tap[t], u32)
            v32 = jnp.where(dv == t, tap[t], v32)
        ku[:, cols] = u32
        kv[:, cols] = v32
        for u in range(4):
            chosen = jnp.where(col_block == u + 1, 1, 0)
            if u == 2:
                chosen = chosen + jnp.where(col_block == 0, 1, 0) * has_left
            if u == 1:
                chosen = chosen + jnp.where(col_block == 5, 1, 0) * has_right
            kv_wide[32 * u : 32 * u + 32, cols] = jnp.where(chosen > 0, v32, 0.0).astype(bf16)

    arrive(q_in, 1)
    for k in range(GRPS):
        arrived = q_in[k].astype(f32)
        q_all[8 * k : 8 * k + 8, :] = arrived[:, :128]
        q_all[8 * GRPS + 8 * k : 8 * GRPS + 8 * k + 8, :] = arrived[:, 128:]
    stacked = []
    for k in range(8):
        stacked.append(q_all[pl.ds(k, 2 * GRPS, stride=8), :].astype(bf16))
    mixed = mm(first[...], jnp.concatenate(stacked, axis=1))
    cos, sin = twist[:, :128], twist[:, 128:]
    both = []
    for k in range(8):
        mixed_re = mixed[:128, 128 * k : 128 * k + 128]
        mixed_im = mixed[128:, 128 * k : 128 * k + 128]
        pair = [mixed_re * cos + mixed_im * sin, mixed_im * cos - mixed_re * sin]
        both.append(jnp.concatenate(pair, axis=1).astype(bf16))
    waves = mm_t(second[grp], jnp.concatenate(both, axis=0))
    for k in range(8):
        u_all[8 * k : 8 * k + 8, :] = waves[:, 128 * k : 128 * k + 128]
    for k in range(ROLES):
        pair = [u_all[pl.ds(2 * k + c, 8, stride=8), :] for c in range(2)]
        u_out[k] = jnp.concatenate(pair, axis=1).astype(bf16)

    keep(u_out.at[role], s_in.at[slot], 2)

    def send_rows(i, _):
        device = near_peer(i)
        push(u_out.at[device[0]], s_in.at[slot], 2, device)
        return 0

    lax.fori_loop(1, NEAR, send_rows, 0)
    arrive(s_in, 2)

    for k in range(NEAR):
        arrived = s_in[k].astype(f32)
        for c in range(2):
            s_all[128 * c + 8 * k : 128 * c + 8 * k + 8, :] = arrived[:, 128 * c : 128 * c + 128]
    slots = lax.broadcasted_iota(jnp.int32, (1, KMAX), 1)
    total = [[jnp.zeros((8, 128), f32) for _ in range(4)] for _ in range(3)]
    for k, p in patches:
        cols = slice(KMAX * (NP_LOCAL * k + p), KMAX * (NP_LOCAL * k + p + 1))
        row_block, col_block = block_of(k, p, 128)
        rows = []
        for m in range(8):
            block = s_all[32 * m : 32 * m + 8, :]
            for h in range(1, 4):
                at = slice(32 * m + 8 * h, 32 * m + 8 * h + 8)
                block = jnp.where(row_block == h, s_all[at, :], block)
            rows.append(block)
        along = mm(jnp.concatenate(rows, axis=0).astype(bf16), kv_wide[:, cols])
        live = slots < jnp.broadcast_to(counts[k, 0:1, p : p + 1], (1, KMAX))
        ku_p = ku[:, cols]
        kv_p = kv[:, cols]
        weighted = []
        for c in range(2):
            predicted = jnp.sum(along[32 * c : 32 * c + 32] * ku_p, axis=0, keepdims=True)
            left_over = jnp.where(live, observed[k, c, 0, p : p + 1, :] - predicted, 0.0)
            left[k, c, 0, p : p + 1, :] = left_over
            weighted.append((kv_p * left_over).astype(bf16))
        mine_u = ku[pl.ds(pl.multiple_of(8 * rep, 8), 8), cols].astype(bf16)
        both = mm_t(mine_u, jnp.concatenate(weighted + weighted, axis=0))
        turned = pltpu.roll(both, 32, 1)
        even = (lane // 32) % 2 == 0
        pieces = (
            (jnp.where(even, both, turned), lane // 32 == col_block - 1),
            (jnp.where(even, turned, both), lane // 32 == col_block - 1),
            (
                jnp.where((lane < 32) | (lane >= 96), both, turned),
                jnp.where(even, 0, 5) == col_block,
            ),
        )
        for j, (piece, inside) in enumerate(pieces):
            for h in range(4):
                here = jnp.where(row_block == h, 1, 0) * jnp.where(inside, 1, 0)
                total[j][h] = total[j][h] + jnp.where(here > 0, piece, 0.0)

    z_all[pl.ds(3, GRPS, stride=4), :] = jnp.zeros((GRPS, 128), f32)
    for k in range(3):
        z_all[pl.ds(k, GRPS, stride=4), :] = jnp.concatenate(total[k], axis=0)
    for k in range(GRPS):
        z_out[k] = z_all[4 * k : 4 * k + 4, :].astype(bf16)
    keep(z_out.at[grp], z_in.at[sub], 3)

    def send_owner(to):
        for k in range(ROLES):
            push(z_out.at[to], z_in.at[sub], 3, (lax.rem(role + k, ROLES), to, rep))

    def send_early(i, _):
        to = i

        @pl.when(to != grp)
        def _():
            push(z_out.at[to], z_in.at[sub], 3, (role, to, rep))

        for k in range(1, ROLES):
            push(z_out.at[to], z_in.at[sub], 3, (lax.rem(role + k, ROLES), to, rep))
        return 0

    lax.fori_loop(0, GRPS, send_early, 0)
    residual[...] = left[rep]
    arrive(z_in, 3)

    for k in range(C):
        z_all[4 * k : 4 * k + 4, :] = z_in[k].astype(f32)
    owned = [z_all[pl.ds(k, C, stride=4), :] for k in range(3)]
    edges = owned[2]
    column = lax.broadcasted_iota(jnp.int32, (C, 128), 1)
    subgrid = lax.broadcasted_iota(jnp.int32, (C, 128), 0)
    for c in range(2):
        side = pltpu.roll(edges, 96 if c == 0 else 32, 1)
        from_left = jnp.where((column < 32) & (subgrid > 0), pltpu.roll(side, 1, 0), 0.0)
        from_right = jnp.where((column >= 96) & (subgrid < C - 1), pltpu.roll(side, C - 1, 0), 0.0)
        returned[c] = (owned[c] + from_left + from_right).astype(bf16)

    drain(x_in, NEAR - 1, 0)
    drain(q_in, GRPS - 1, 1)
    drain(s_in, NEAR - 1, 2)
    drain(z_in, C - 1, 3)
    for k, held in enumerate(shared):
        drain(held, REPS - 1, 4 + k)


def flush(residual, returned, residual_out, returned_out, done):
    copies = [
        pltpu.make_async_copy(returned, returned_out, done.at[0]),
        pltpu.make_async_copy(residual, residual_out, done.at[1]),
    ]
    for copy in copies:
        copy.start()
    for copy in copies:
        copy.wait()


def local(facets, taper, kernel, observed, patch_pos, counts, vis_u, vis_v):
    vmem = pl.BlockSpec(memory_space=pltpu.VMEM)
    hbm = pl.BlockSpec(memory_space=pltpu.HBM)
    residual, returned = pl.pallas_call(
        body,
        out_shape=(
            pltpu.VMEM((2, 1, NP_LOCAL, KMAX), f32),
            pltpu.VMEM((2, C, C), bf16),
        ),
        in_specs=[hbm] * 13,
        out_specs=(vmem, vmem),
        scratch_shapes=[
            pltpu.VMEM((2, 32, F), bf16),
            pltpu.VMEM((1, F), f32),
            pltpu.VMEM((128, 256), bf16),
            pltpu.VMEM((32, 256), f32),
            pltpu.VMEM((256, 64), bf16),
            pltpu.VMEM((128, 256), f32),
            pltpu.VMEM((GRPS, 8, 256), bf16),
            pltpu.VMEM((1, KW), f32),
            pltpu.VMEM((REPS, 2, 1, NP_LOCAL, KMAX), f32),
            pltpu.VMEM((REPS, 1, NP_LOCAL), jnp.int32),
            pltpu.VMEM((REPS, 1, NP_LOCAL), jnp.int32),
            pltpu.VMEM((REPS, 1, NP_LOCAL, KMAX), jnp.int32),
            pltpu.VMEM((REPS, 1, NP_LOCAL, KMAX), jnp.int32),
            pltpu.VMEM((NEAR, 8, 128), bf16),
            pltpu.VMEM((NEAR, 8, 128), bf16),
            pltpu.VMEM((1, 8, 256), bf16),
            pltpu.VMEM((GRPS, 8, 256), bf16),
            pltpu.VMEM((16 * GRPS, 128), f32),
            pltpu.VMEM((64, 128), f32),
            pltpu.VMEM((ROLES, 8, 256), bf16),
            pltpu.VMEM((NEAR, 8, 256), bf16),
            pltpu.VMEM((4 * C, 128), f32),
            pltpu.VMEM((GRPS, 4, 128), bf16),
            pltpu.VMEM((C, 4, 128), bf16),
            pltpu.VMEM((2 * C, 128), f32),
            pltpu.VMEM((REPS, 2, 1, NP_LOCAL, KMAX), f32),
            pltpu.VMEM((PATCH, REPS * NP_LOCAL * KMAX), f32),
            pltpu.VMEM((PATCH, REPS * NP_LOCAL * KMAX), f32),
            pltpu.VMEM((C, REPS * NP_LOCAL * KMAX), bf16),
            pltpu.SemaphoreType.DMA((9,)),
            pltpu.SemaphoreType.DMA((9,)),
            pltpu.SemaphoreType.DMA((16,)),
        ],
        compiler_params=pltpu.CompilerParams(
            collective_id=0, has_side_effects=True
        ),
        name="cycle",
    )(facets, taper, *tables(), kernel[None], observed, patch_pos, counts, vis_u, vis_v)
    anywhere = pl.BlockSpec(memory_space=pl.ANY)
    residual, returned = pl.pallas_call(
        flush,
        out_shape=(
            jax.ShapeDtypeStruct((2, 1, NP_LOCAL, KMAX), f32),
            jax.ShapeDtypeStruct((2, C, C), bf16),
        ),
        in_specs=[vmem, vmem],
        out_specs=(anywhere, anywhere),
        scratch_shapes=[pltpu.SemaphoreType.DMA((2,))],
        compiler_params=pltpu.CompilerParams(vmem_limit_bytes=1 << 20),
        name="flush",
    )(residual, returned)
    return residual, returned.reshape(2, C, 1, C)


def solution(mesh):
    both = ("role", "grp")
    return jax.shard_map(
        local,
        mesh=mesh,
        in_specs=(
            P("role", None, ("grp", "rep"), None),
            P("role", None),
            P(),
            P(None, both, "rep", None),
            P(both, "rep"),
            P(both, "rep"),
            P(both, "rep", None),
            P(both, "rep", None),
        ),
        out_specs=(P(None, both, "rep", None), P(None, None, ("grp", "rep"), None)),
        check_vma=False,
    )
```

```python
import math

import jax
import jax.numpy as jnp
import numpy as np
from jax import lax
from jax.experimental import pallas as pl
from jax.experimental.pallas import tpu as pltpu
from jax.sharding import PartitionSpec as P

F = 4096
C = 128
PATCH = 32
KW = 8
NP_LOCAL = 4
KMAX = 512
ROLES = 4
GRPS = 32
REPS = 4
NEAR = ROLES * REPS
MESH = pl.DeviceIdType.MESH
bf16 = jnp.bfloat16
f32 = jnp.float32


def row_order():
    place = np.arange(C)
    return 4 * (place % GRPS) + place // GRPS


def tables():
    turn = 2.0 * math.pi
    row = row_order()
    cell = np.arange(128)
    block = np.arange(32)
    angle = turn * ((cell[:, None] * row[None, :]) % F) / F
    near = np.concatenate([np.cos(angle), -np.sin(angle)], axis=1)
    angle = turn * ((block[:, None] * row[None, :]) % 32) / 32
    far = np.concatenate([np.cos(angle), -np.sin(angle)], axis=1) / math.sqrt(F)
    angle = turn * ((cell[:, None] * block[None, :]) % 32) / 32
    cos, sin = np.cos(angle), np.sin(angle)
    first = np.block([[cos, sin], [-sin, cos]])
    angle = turn * ((cell[:, None] * cell[None, :]) % F) / F
    twist = np.concatenate([np.cos(angle), np.sin(angle)], axis=1)
    angle = turn * ((cell[:, None] * cell[None, :]) % 128) / 128
    cos, sin = np.cos(angle) / math.sqrt(F), np.sin(angle) / math.sqrt(F)
    second = np.stack([np.concatenate([cos, sin], 1), np.concatenate([-sin, cos], 1)], axis=1)
    second = second.reshape(ROLES, GRPS, 2, 256).transpose(1, 0, 2, 3).reshape(GRPS, 8, 256)
    return (
        jnp.asarray(near, bf16),
        jnp.asarray(far, f32),
        jnp.asarray(first, bf16),
        jnp.asarray(twist, f32),
        jnp.asarray(second, bf16),
    )


def mm(left, right):
    return lax.dot_general(left, right, (((1,), (0,)), ((), ())), preferred_element_type=f32)


def mm_t(left, right):
    return lax.dot_general(left, right, (((1,), (1,)), ((), ())), preferred_element_type=f32)


def body(
    facets_far, taper_far, near_far, far_far, first_far, twist_far, second_far,
    taps_far, observed_far, patch_pos_far, counts_far, vis_u_far, vis_v_far,
    residual, returned,
    facets, taper, near, far, first, twist, second,
    taps, observed, patch_pos, counts, vis_u, vis_v,
    x_out, x_in, q_out, q_in, q_all, u_all, u_out, s_in,
    z_all, z_out, z_in, s_all, left,
    ku, kv, kv_wide,
    sent, got, loaded,
):
    role, grp, rep = lax.axis_index("role"), lax.axis_index("grp"), lax.axis_index("rep")

    def near_peer(i):
        return (lax.rem(role + i // REPS, ROLES), grp, lax.rem(rep + i % REPS, REPS))

    def grp_peer(i):
        return lax.rem(grp + i, GRPS)

    def for_grps(send):
        for dz in (2, 1, 3):
            base = lax.rem(grp // 8 + dz, 4) * 8

            def step(i, _, base=base):
                send(base + lax.rem(grp + i, 8))
                return 0

            lax.fori_loop(3, 11, step, 0)

        def last(i, _):
            send((grp // 8) * 8 + lax.rem(grp + 1 + lax.rem(i, 7), 8))
            return 0

        lax.fori_loop(2, 9, last, 0)

    inputs = [
        (taper_far, taper), (near_far, near), (far_far, far),
        (first_far, first), (twist_far, twist), (second_far, second), (taps_far, taps),
        (observed_far, observed.at[rep]), (patch_pos_far, patch_pos.at[rep]),
        (counts_far, counts.at[rep]), (vis_u_far, vis_u.at[rep]), (vis_v_far, vis_v.at[rep]),
    ]
    loads = []
    for k in range(4):
        part = pl.ds(1024 * k, 1024)
        loads.append((facets_far.at[0, :, :, part], facets.at[:, :, part]))
    loads = [
        pltpu.make_async_copy(src, dst, loaded.at[k]) for k, (src, dst) in enumerate(loads + inputs)
    ]
    for load in loads[4:7] + loads[:4] + loads[7:]:
        load.start()

    barrier = pltpu.get_barrier_semaphore()

    def greet_near(i, _):
        pl.semaphore_signal(barrier, inc=1, device_id=near_peer(i), device_id_type=MESH)
        return 0

    def greet_grp(i, _):
        pl.semaphore_signal(barrier, inc=1, device_id=(role, grp_peer(i), rep), device_id_type=MESH)
        return 0

    lax.fori_loop(1, GRPS, greet_grp, 0)
    lax.fori_loop(1, NEAR, greet_near, 0)

    def push(src, dst, phase, device):
        pltpu.make_async_remote_copy(
            src_ref=src, dst_ref=dst, send_sem=sent.at[phase], recv_sem=got.at[phase],
            device_id=device, device_id_type=MESH,
        ).start()

    def keep(src, dst, phase):
        pltpu.make_async_copy(src, dst, got.at[phase]).start()

    def arrive(buffer, phase):
        pltpu.make_async_copy(buffer, buffer, got.at[phase]).wait()

    def drain(buffer, count, phase):
        part = buffer.at[pl.ds(0, count)]
        pltpu.make_async_copy(part, part, sent.at[phase]).wait()

    for load in loads[:7]:
        load.wait()
    table = near[...]
    part_re = jnp.zeros((32, C), f32)
    part_im = jnp.zeros((32, C), f32)
    for chunk in range(4):
        blocks = []
        for i in range(8 * chunk, 8 * chunk + 8):
            at = slice(128 * i, 128 * i + 128)
            blocks += [(facets[c, :, at].astype(f32) * taper[:, at]).astype(bf16) for c in range(2)]
        spectrum = mm(jnp.concatenate(blocks, axis=0), table)
        for k in range(8):
            i = 8 * chunk + k
            of_re = spectrum[64 * k : 64 * k + 32]
            of_im = spectrum[64 * k + 32 : 64 * k + 64]
            t_re = of_re[:, :C] - of_im[:, C:]
            t_im = of_re[:, C:] + of_im[:, :C]
            e_re = far[i : i + 1, :C]
            e_im = far[i : i + 1, C:]
            part_re = part_re + (t_re * e_re - t_im * e_im)
            part_im = part_im + (t_re * e_im + t_im * e_re)
    turned = jnp.concatenate([part_re, part_im, part_re, part_im], axis=0).T
    lane = lax.broadcasted_iota(jnp.int32, (1, 128), 1)
    own = taper[:, pl.ds(pl.multiple_of(grp * 128, 128), 128)]
    mine = jnp.zeros((1, 128), f32)
    for r in range(REPS):
        moved = own if r == 0 else pltpu.roll(own, 128 - 32 * r, 1)
        mine = mine + moved * jnp.where(rep == r, 1.0, 0.0)
    mine = jnp.where(lane < 32, mine, 0.0)
    mine = mine + pltpu.roll(mine, 32, 1)
    mine = mine + pltpu.roll(mine, 64, 1)
    turned = turned * mine
    for k in range(NEAR):
        x_out[k] = turned[8 * k : 8 * k + 8].astype(bf16)

    pl.semaphore_wait(barrier, GRPS + NEAR - 2)

    slot = role * REPS + rep

    def spread(out, into, phase):
        keep(out.at[slot], into.at[slot], phase)

        def send(i, _):
            device = near_peer(i)
            push(out.at[device[0] * REPS + device[2]], into.at[slot], phase, device)
            return 0

        lax.fori_loop(1, NEAR, send, 0)

    spread(x_out, x_in, 0)
    arrive(x_in, 0)
    cell_re = jnp.zeros((8, 128), f32)
    cell_im = jnp.zeros((8, 128), f32)
    for r in range(REPS):
        total = x_in[r].astype(f32)
        for k in range(1, ROLES):
            total = total + x_in[k * REPS + r].astype(f32)
        inside = (lane >= 32 * r) & (lane < 32 * r + 32)
        moved = pltpu.roll(total, 32, 1)
        cell_re = jnp.where(inside, total if r % 2 == 0 else moved, cell_re)
        cell_im = jnp.where(inside, moved if r % 2 == 0 else total, cell_im)
    q_out[0] = jnp.concatenate([cell_re, cell_im], axis=1).astype(bf16)
    keep(q_out.at[0], q_in.at[grp], 1)

    def send_cells(to):
        push(q_out.at[0], q_in.at[grp], 1, (role, to, rep))

    for_grps(send_cells)

    for load in loads[7:]:
        load.wait()
    shared = (observed, patch_pos, counts, vis_u, vis_v)
    for k, held in enumerate(shared):

        def send_held(i, _, held=held, k=k):
            push(held.at[rep], held.at[rep], 4 + k, (role, grp, lax.rem(rep + i, REPS)))
            return 0

        lax.fori_loop(1, REPS, send_held, 0)
    for k, held in enumerate(shared):
        part = held.at[pl.ds(0, REPS - 1)]
        pltpu.make_async_copy(part, part, got.at[4 + k]).wait()

    sub = role * GRPS + grp
    place = lax.broadcasted_iota(jnp.int32, (PATCH, KMAX), 0)
    row_in_patch = 4 * (place % 8) + place // 8
    has_left = jnp.where(sub > 0, 1, 0)
    has_right = jnp.where(sub < ROLES * GRPS - 1, 1, 0)

    def block_of(k, p, width):
        position = jnp.broadcast_to(patch_pos[k, 0:1, p : p + 1], (1, width))
        row_block = (
            jnp.where(position >= 6, 1, 0)
            + jnp.where(position >= 12, 1, 0)
            + jnp.where(position >= 18, 1, 0)
        )
        return row_block, position - 6 * row_block

    patches = [(k, p) for k in range(REPS) for p in range(NP_LOCAL)]
    tap = [jnp.broadcast_to(taps[0:1, t : t + 1], (PATCH, KMAX)) for t in range(KW)]
    for k, p in patches:
        cols = slice(KMAX * (NP_LOCAL * k + p), KMAX * (NP_LOCAL * k + p + 1))
        _, col_block = block_of(k, p, KMAX)
        du = row_in_patch - vis_u[k, 0, p : p + 1, :]
        dv = place - vis_v[k, 0, p : p + 1, :]
        u32 = jnp.zeros((PATCH, KMAX), f32)
        v32 = jnp.zeros((PATCH, KMAX), f32)
        for t in range(KW):
            u32 = jnp.where(du == t, tap[t], u32)
            v32 = jnp.where(dv == t, tap[t], v32)
        ku[:, cols] = u32
        kv[:, cols] = v32
        for u in range(4):
            chosen = jnp.where(col_block == u + 1, 1, 0)
            if u == 2:
                chosen = chosen + jnp.where(col_block == 0, 1, 0) * has_left
            if u == 1:
                chosen = chosen + jnp.where(col_block == 5, 1, 0) * has_right
            kv_wide[32 * u : 32 * u + 32, cols] = jnp.where(chosen > 0, v32, 0.0).astype(bf16)

    arrive(q_in, 1)
    for k in range(GRPS):
        arrived = q_in[k].astype(f32)
        q_all[8 * k : 8 * k + 8, :] = arrived[:, :128]
        q_all[8 * GRPS + 8 * k : 8 * GRPS + 8 * k + 8, :] = arrived[:, 128:]
    stacked = []
    for k in range(8):
        stacked.append(q_all[pl.ds(k, 2 * GRPS, stride=8), :].astype(bf16))
    mixed = mm(first[...], jnp.concatenate(stacked, axis=1))
    cos, sin = twist[:, :128], twist[:, 128:]
    both = []
    for k in range(8):
        mixed_re = mixed[:128, 128 * k : 128 * k + 128]
        mixed_im = mixed[128:, 128 * k : 128 * k + 128]
        pair = [mixed_re * cos + mixed_im * sin, mixed_im * cos - mixed_re * sin]
        both.append(jnp.concatenate(pair, axis=1).astype(bf16))
    waves = mm_t(second[grp], jnp.concatenate(both, axis=0))
    for k in range(8):
        u_all[8 * k : 8 * k + 8, :] = waves[:, 128 * k : 128 * k + 128]
    for k in range(ROLES):
        pair = [u_all[pl.ds(2 * k + c, 8, stride=8), :] for c in range(2)]
        u_out[k] = jnp.concatenate(pair, axis=1).astype(bf16)

    keep(u_out.at[role], s_in.at[slot], 2)

    def send_rows(i, _):
        device = near_peer(i)
        push(u_out.at[device[0]], s_in.at[slot], 2, device)
        return 0

    lax.fori_loop(1, NEAR, send_rows, 0)
    arrive(s_in, 2)

    for k in range(NEAR):
        arrived = s_in[k].astype(f32)
        for c in range(2):
            s_all[128 * c + 8 * k : 128 * c + 8 * k + 8, :] = arrived[:, 128 * c : 128 * c + 128]
    slots = lax.broadcasted_iota(jnp.int32, (1, KMAX), 1)
    total = [[jnp.zeros((8, 128), f32) for _ in range(4)] for _ in range(3)]
    def columns(k, p):
        return slice(KMAX * (NP_LOCAL * k + p), KMAX * (NP_LOCAL * k + p + 1))

    for k in range(REPS):
        predicted = [[], []]
        live = []
        for p in range(NP_LOCAL):
            row_block, _ = block_of(k, p, 128)
            rows = []
            for m in range(8):
                block = s_all[32 * m : 32 * m + 8, :]
                for h in range(1, 4):
                    at = slice(32 * m + 8 * h, 32 * m + 8 * h + 8)
                    block = jnp.where(row_block == h, s_all[at, :], block)
                rows.append(block)
            along = mm(jnp.concatenate(rows, axis=0).astype(bf16), kv_wide[:, columns(k, p)])
            ku_p = ku[:, columns(k, p)]
            for c in range(2):
                product = along[32 * c : 32 * c + 32] * ku_p
                predicted[c].append(jnp.sum(product, axis=0, keepdims=True))
            live.append(jnp.broadcast_to(counts[k, 0:1, p : p + 1], (1, KMAX)))
        alive = slots < jnp.concatenate(live, axis=0)
        for c in range(2):
            over = observed[k, c, 0] - jnp.concatenate(predicted[c], axis=0)
            left[k, c, 0] = jnp.where(alive, over, 0.0)
    for k, p in patches:
        cols = columns(k, p)
        row_block, col_block = block_of(k, p, 128)
        kv_p = kv[:, cols]
        weighted = [(kv_p * left[k, c, 0, p : p + 1, :]).astype(bf16) for c in range(2)]
        mine_u = ku[pl.ds(pl.multiple_of(8 * rep, 8), 8), cols].astype(bf16)
        both = mm_t(mine_u, jnp.concatenate(weighted + weighted, axis=0))
        turned = pltpu.roll(both, 32, 1)
        even = (lane // 32) % 2 == 0
        pieces = (
            (jnp.where(even, both, turned), lane // 32 == col_block - 1),
            (jnp.where(even, turned, both), lane // 32 == col_block - 1),
            (
                jnp.where((lane < 32) | (lane >= 96), both, turned),
                jnp.where(even, 0, 5) == col_block,
            ),
        )
        for j, (piece, inside) in enumerate(pieces):
            for h in range(4):
                here = jnp.where(row_block == h, 1, 0) * jnp.where(inside, 1, 0)
                total[j][h] = total[j][h] + jnp.where(here > 0, piece, 0.0)

    z_all[pl.ds(3, GRPS, stride=4), :] = jnp.zeros((GRPS, 128), f32)
    for k in range(3):
        z_all[pl.ds(k, GRPS, stride=4), :] = jnp.concatenate(total[k], axis=0)
    for k in range(GRPS):
        z_out[k] = z_all[4 * k : 4 * k + 4, :].astype(bf16)
    keep(z_out.at[grp], z_in.at[sub], 3)

    def send_owner(to):
        for k in range(ROLES):
            push(z_out.at[to], z_in.at[sub], 3, (lax.rem(role + k, ROLES), to, rep))

    def send_early(i, _):
        to = i

        @pl.when(to != grp)
        def _():
            push(z_out.at[to], z_in.at[sub], 3, (role, to, rep))

        for k in range(1, ROLES):
            push(z_out.at[to], z_in.at[sub], 3, (lax.rem(role + k, ROLES), to, rep))
        return 0

    lax.fori_loop(0, GRPS, send_early, 0)
    residual[...] = left[rep]
    arrive(z_in, 3)

    for k in range(C):
        z_all[4 * k : 4 * k + 4, :] = z_in[k].astype(f32)
    owned = [z_all[pl.ds(k, C, stride=4), :] for k in range(3)]
    edges = owned[2]
    column = lax.broadcasted_iota(jnp.int32, (C, 128), 1)
    subgrid = lax.broadcasted_iota(jnp.int32, (C, 128), 0)
    for c in range(2):
        side = pltpu.roll(edges, 96 if c == 0 else 32, 1)
        from_left = jnp.where((column < 32) & (subgrid > 0), pltpu.roll(side, 1, 0), 0.0)
        from_right = jnp.where((column >= 96) & (subgrid < C - 1), pltpu.roll(side, C - 1, 0), 0.0)
        returned[c] = (owned[c] + from_left + from_right).astype(bf16)

    drain(x_in, NEAR - 1, 0)
    drain(q_in, GRPS - 1, 1)
    drain(s_in, NEAR - 1, 2)
    drain(z_in, C - 1, 3)
    for k, held in enumerate(shared):
        drain(held, REPS - 1, 4 + k)


def flush(residual, returned, residual_out, returned_out, done):
    copies = [
        pltpu.make_async_copy(returned, returned_out, done.at[0]),
        pltpu.make_async_copy(residual, residual_out, done.at[1]),
    ]
    for copy in copies:
        copy.start()
    for copy in copies:
        copy.wait()


def local(facets, taper, kernel, observed, patch_pos, counts, vis_u, vis_v):
    vmem = pl.BlockSpec(memory_space=pltpu.VMEM)
    hbm = pl.BlockSpec(memory_space=pltpu.HBM)
    residual, returned = pl.pallas_call(
        body,
        out_shape=(
            pltpu.VMEM((2, 1, NP_LOCAL, KMAX), f32),
            pltpu.VMEM((2, C, C), bf16),
        ),
        in_specs=[hbm] * 13,
        out_specs=(vmem, vmem),
        scratch_shapes=[
            pltpu.VMEM((2, 32, F), bf16),
            pltpu.VMEM((1, F), f32),
            pltpu.VMEM((128, 256), bf16),
            pltpu.VMEM((32, 256), f32),
            pltpu.VMEM((256, 64), bf16),
            pltpu.VMEM((128, 256), f32),
            pltpu.VMEM((GRPS, 8, 256), bf16),
            pltpu.VMEM((1, KW), f32),
            pltpu.VMEM((REPS, 2, 1, NP_LOCAL, KMAX), f32),
            pltpu.VMEM((REPS, 1, NP_LOCAL), jnp.int32),
            pltpu.VMEM((REPS, 1, NP_LOCAL), jnp.int32),
            pltpu.VMEM((REPS, 1, NP_LOCAL, KMAX), jnp.int32),
            pltpu.VMEM((REPS, 1, NP_LOCAL, KMAX), jnp.int32),
            pltpu.VMEM((NEAR, 8, 128), bf16),
            pltpu.VMEM((NEAR, 8, 128), bf16),
            pltpu.VMEM((1, 8, 256), bf16),
            pltpu.VMEM((GRPS, 8, 256), bf16),
            pltpu.VMEM((16 * GRPS, 128), f32),
            pltpu.VMEM((64, 128), f32),
            pltpu.VMEM((ROLES, 8, 256), bf16),
            pltpu.VMEM((NEAR, 8, 256), bf16),
            pltpu.VMEM((4 * C, 128), f32),
            pltpu.VMEM((GRPS, 4, 128), bf16),
            pltpu.VMEM((C, 4, 128), bf16),
            pltpu.VMEM((2 * C, 128), f32),
            pltpu.VMEM((REPS, 2, 1, NP_LOCAL, KMAX), f32),
            pltpu.VMEM((PATCH, REPS * NP_LOCAL * KMAX), f32),
            pltpu.VMEM((PATCH, REPS * NP_LOCAL * KMAX), f32),
            pltpu.VMEM((C, REPS * NP_LOCAL * KMAX), bf16),
            pltpu.SemaphoreType.DMA((9,)),
            pltpu.SemaphoreType.DMA((9,)),
            pltpu.SemaphoreType.DMA((16,)),
        ],
        compiler_params=pltpu.CompilerParams(
            collective_id=0, has_side_effects=True
        ),
        name="cycle",
    )(facets, taper, *tables(), kernel[None], observed, patch_pos, counts, vis_u, vis_v)
    anywhere = pl.BlockSpec(memory_space=pl.ANY)
    residual, returned = pl.pallas_call(
        flush,
        out_shape=(
            jax.ShapeDtypeStruct((2, 1, NP_LOCAL, KMAX), f32),
            jax.ShapeDtypeStruct((2, C, C), bf16),
        ),
        in_specs=[vmem, vmem],
        out_specs=(anywhere, anywhere),
        scratch_shapes=[pltpu.SemaphoreType.DMA((2,))],
        compiler_params=pltpu.CompilerParams(vmem_limit_bytes=1 << 20),
        name="flush",
    )(residual, returned)
    return residual, returned.reshape(2, C, 1, C)


def solution(mesh):
    both = ("role", "grp")
    return jax.shard_map(
        local,
        mesh=mesh,
        in_specs=(
            P("role", None, ("grp", "rep"), None),
            P("role", None),
            P(),
            P(None, both, "rep", None),
            P(both, "rep"),
            P(both, "rep"),
            P(both, "rep", None),
            P(both, "rep", None),
        ),
        out_specs=(P(None, both, "rep", None), P(None, None, ("grp", "rep"), None)),
        check_vma=False,
    )
```

```python
import math

import jax
import jax.numpy as jnp
import numpy as np
from jax import lax
from jax.experimental import pallas as pl
from jax.experimental.pallas import tpu as pltpu
from jax.sharding import PartitionSpec as P

F = 4096
C = 128
PATCH = 32
KW = 8
NP_LOCAL = 4
KMAX = 512
ROLES = 4
GRPS = 32
REPS = 4
NEAR = ROLES * REPS
MESH = pl.DeviceIdType.MESH
bf16 = jnp.bfloat16
f32 = jnp.float32


def row_order():
    place = np.arange(C)
    return 4 * (place % GRPS) + place // GRPS


def tables():
    turn = 2.0 * math.pi
    row = row_order()
    cell = np.arange(128)
    block = np.arange(32)
    angle = turn * ((cell[:, None] * row[None, :]) % F) / F
    near = np.concatenate([np.cos(angle), -np.sin(angle)], axis=1)
    angle = turn * ((block[:, None] * row[None, :]) % 32) / 32
    far = np.concatenate([np.cos(angle), -np.sin(angle)], axis=1) / math.sqrt(F)
    angle = turn * ((cell[:, None] * block[None, :]) % 32) / 32
    cos, sin = np.cos(angle), np.sin(angle)
    first = np.block([[cos, sin], [-sin, cos]])
    angle = turn * ((cell[:, None] * cell[None, :]) % F) / F
    twist = np.concatenate([np.cos(angle), np.sin(angle)], axis=1)
    angle = turn * ((cell[:, None] * cell[None, :]) % 128) / 128
    cos, sin = np.cos(angle) / math.sqrt(F), np.sin(angle) / math.sqrt(F)
    second = np.stack([np.concatenate([cos, sin], 1), np.concatenate([-sin, cos], 1)], axis=1)
    second = second.reshape(ROLES, GRPS, 2, 256).transpose(1, 0, 2, 3).reshape(GRPS, 8, 256)
    return (
        jnp.asarray(near, bf16),
        jnp.asarray(far, f32),
        jnp.asarray(first, bf16),
        jnp.asarray(twist, f32),
        jnp.asarray(second, bf16),
    )


def mm(left, right):
    return lax.dot_general(left, right, (((1,), (0,)), ((), ())), preferred_element_type=f32)


def mm_t(left, right):
    return lax.dot_general(left, right, (((1,), (1,)), ((), ())), preferred_element_type=f32)


def body(
    facets_far, taper_far, near_far, far_far, first_far, twist_far, second_far,
    taps_far, observed_far, patch_pos_far, counts_far, vis_u_far, vis_v_far,
    residual, returned,
    facets, taper, near, far, first, twist, second,
    taps, observed, patch_pos, counts, vis_u, vis_v,
    x_out, x_in, q_out, q_in, q_all, u_all, u_out, s_in,
    z_all, z_out, z_in, s_all, left,
    ku, kv, kv_wide,
    sent, got, loaded,
):
    role, grp, rep = lax.axis_index("role"), lax.axis_index("grp"), lax.axis_index("rep")

    def near_peer(i):
        return (lax.rem(role + i // REPS + 2, ROLES), grp, lax.rem(rep + i % REPS + 2, REPS))

    def grp_peer(i):
        return lax.rem(grp + i, GRPS)

    def for_grps(send):
        for dz in (2, 1, 3):
            base = lax.rem(grp // 8 + dz, 4) * 8

            def step(i, _, base=base):
                send(base + lax.rem(grp + i, 8))
                return 0

            lax.fori_loop(3, 11, step, 0)

        def last(i, _):
            send((grp // 8) * 8 + lax.rem(grp + 1 + lax.rem(i, 7), 8))
            return 0

        lax.fori_loop(2, 9, last, 0)

    inputs = [
        (taper_far, taper), (near_far, near), (far_far, far),
        (first_far, first), (twist_far, twist), (second_far, second), (taps_far, taps),
        (observed_far, observed.at[rep]), (patch_pos_far, patch_pos.at[rep]),
        (counts_far, counts.at[rep]), (vis_u_far, vis_u.at[rep]), (vis_v_far, vis_v.at[rep]),
    ]
    loads = []
    for k in range(4):
        part = pl.ds(1024 * k, 1024)
        loads.append((facets_far.at[0, :, :, part], facets.at[:, :, part]))
    loads = [
        pltpu.make_async_copy(src, dst, loaded.at[k]) for k, (src, dst) in enumerate(loads + inputs)
    ]
    for load in loads[4:7] + loads[:4] + loads[7:]:
        load.start()

    barrier = pltpu.get_barrier_semaphore()

    def greet_near(i, _):
        pl.semaphore_signal(barrier, inc=1, device_id=near_peer(i), device_id_type=MESH)
        return 0

    def greet_grp(i, _):
        pl.semaphore_signal(barrier, inc=1, device_id=(role, grp_peer(i), rep), device_id_type=MESH)
        return 0

    lax.fori_loop(1, GRPS, greet_grp, 0)
    lax.fori_loop(0, 10, greet_near, 0)
    lax.fori_loop(11, NEAR, greet_near, 0)

    def push(src, dst, phase, device):
        pltpu.make_async_remote_copy(
            src_ref=src, dst_ref=dst, send_sem=sent.at[phase], recv_sem=got.at[phase],
            device_id=device, device_id_type=MESH,
        ).start()

    def keep(src, dst, phase):
        pltpu.make_async_copy(src, dst, got.at[phase]).start()

    def arrive(buffer, phase):
        pltpu.make_async_copy(buffer, buffer, got.at[phase]).wait()

    def drain(buffer, count, phase):
        part = buffer.at[pl.ds(0, count)]
        pltpu.make_async_copy(part, part, sent.at[phase]).wait()

    for load in loads[:7]:
        load.wait()
    table = near[...]
    part_re = jnp.zeros((32, C), f32)
    part_im = jnp.zeros((32, C), f32)
    for chunk in range(4):
        blocks = []
        for i in range(8 * chunk, 8 * chunk + 8):
            at = slice(128 * i, 128 * i + 128)
            blocks += [(facets[c, :, at].astype(f32) * taper[:, at]).astype(bf16) for c in range(2)]
        spectrum = mm(jnp.concatenate(blocks, axis=0), table)
        for k in range(8):
            i = 8 * chunk + k
            of_re = spectrum[64 * k : 64 * k + 32]
            of_im = spectrum[64 * k + 32 : 64 * k + 64]
            t_re = of_re[:, :C] - of_im[:, C:]
            t_im = of_re[:, C:] + of_im[:, :C]
            e_re = far[i : i + 1, :C]
            e_im = far[i : i + 1, C:]
            part_re = part_re + (t_re * e_re - t_im * e_im)
            part_im = part_im + (t_re * e_im + t_im * e_re)
    turned = jnp.concatenate([part_re, part_im, part_re, part_im], axis=0).T
    lane = lax.broadcasted_iota(jnp.int32, (1, 128), 1)
    own = taper[:, pl.ds(pl.multiple_of(grp * 128, 128), 128)]
    mine = jnp.zeros((1, 128), f32)
    for r in range(REPS):
        moved = own if r == 0 else pltpu.roll(own, 128 - 32 * r, 1)
        mine = mine + moved * jnp.where(rep == r, 1.0, 0.0)
    mine = jnp.where(lane < 32, mine, 0.0)
    mine = mine + pltpu.roll(mine, 32, 1)
    mine = mine + pltpu.roll(mine, 64, 1)
    turned = turned * mine
    for k in range(NEAR):
        x_out[k] = turned[8 * k : 8 * k + 8].astype(bf16)

    pl.semaphore_wait(barrier, GRPS + NEAR - 2)

    slot = role * REPS + rep

    def spread(out, into, phase):
        keep(out.at[slot], into.at[slot], phase)

        def send(i, _):
            device = near_peer(i)
            push(out.at[device[0] * REPS + device[2]], into.at[slot], phase, device)
            return 0

        lax.fori_loop(0, 10, send, 0)
        lax.fori_loop(11, NEAR, send, 0)

    spread(x_out, x_in, 0)
    arrive(x_in, 0)
    cell_re = jnp.zeros((8, 128), f32)
    cell_im = jnp.zeros((8, 128), f32)
    for r in range(REPS):
        total = x_in[r].astype(f32)
        for k in range(1, ROLES):
            total = total + x_in[k * REPS + r].astype(f32)
        inside = (lane >= 32 * r) & (lane < 32 * r + 32)
        moved = pltpu.roll(total, 32, 1)
        cell_re = jnp.where(inside, total if r % 2 == 0 else moved, cell_re)
        cell_im = jnp.where(inside, moved if r % 2 == 0 else total, cell_im)
    q_out[0] = jnp.concatenate([cell_re, cell_im], axis=1).astype(bf16)
    keep(q_out.at[0], q_in.at[grp], 1)

    def send_cells(to):
        push(q_out.at[0], q_in.at[grp], 1, (role, to, rep))

    for_grps(send_cells)

    for load in loads[7:]:
        load.wait()
    shared = (observed, patch_pos, counts, vis_u, vis_v)
    for k, held in enumerate(shared):

        def send_held(i, _, held=held, k=k):
            push(held.at[rep], held.at[rep], 4 + k, (role, grp, lax.rem(rep + i, REPS)))
            return 0

        lax.fori_loop(1, REPS, send_held, 0)
    for k, held in enumerate(shared):
        part = held.at[pl.ds(0, REPS - 1)]
        pltpu.make_async_copy(part, part, got.at[4 + k]).wait()

    sub = role * GRPS + grp
    place = lax.broadcasted_iota(jnp.int32, (PATCH, KMAX), 0)
    row_in_patch = 4 * (place % 8) + place // 8
    has_left = jnp.where(sub > 0, 1, 0)
    has_right = jnp.where(sub < ROLES * GRPS - 1, 1, 0)

    def block_of(k, p, width):
        position = jnp.broadcast_to(patch_pos[k, 0:1, p : p + 1], (1, width))
        row_block = (
            jnp.where(position >= 6, 1, 0)
            + jnp.where(position >= 12, 1, 0)
            + jnp.where(position >= 18, 1, 0)
        )
        return row_block, position - 6 * row_block

    patches = [(k, p) for k in range(REPS) for p in range(NP_LOCAL)]
    tap = [jnp.broadcast_to(taps[0:1, t : t + 1], (PATCH, KMAX)) for t in range(KW)]
    for k, p in patches:
        cols = slice(KMAX * (NP_LOCAL * k + p), KMAX * (NP_LOCAL * k + p + 1))
        _, col_block = block_of(k, p, KMAX)
        du = row_in_patch - vis_u[k, 0, p : p + 1, :]
        dv = place - vis_v[k, 0, p : p + 1, :]
        u32 = jnp.zeros((PATCH, KMAX), f32)
        v32 = jnp.zeros((PATCH, KMAX), f32)
        for t in range(KW):
            u32 = jnp.where(du == t, tap[t], u32)
            v32 = jnp.where(dv == t, tap[t], v32)
        ku[:, cols] = u32
        kv[:, cols] = v32
        for u in range(4):
            chosen = jnp.where(col_block == u + 1, 1, 0)
            if u == 2:
                chosen = chosen + jnp.where(col_block == 0, 1, 0) * has_left
            if u == 1:
                chosen = chosen + jnp.where(col_block == 5, 1, 0) * has_right
            kv_wide[32 * u : 32 * u + 32, cols] = jnp.where(chosen > 0, v32, 0.0).astype(bf16)

    arrive(q_in, 1)
    for k in range(GRPS):
        arrived = q_in[k].astype(f32)
        q_all[8 * k : 8 * k + 8, :] = arrived[:, :128]
        q_all[8 * GRPS + 8 * k : 8 * GRPS + 8 * k + 8, :] = arrived[:, 128:]
    stacked = []
    for k in range(8):
        stacked.append(q_all[pl.ds(k, 2 * GRPS, stride=8), :].astype(bf16))
    mixed = mm(first[...], jnp.concatenate(stacked, axis=1))
    cos, sin = twist[:, :128], twist[:, 128:]
    both = []
    for k in range(8):
        mixed_re = mixed[:128, 128 * k : 128 * k + 128]
        mixed_im = mixed[128:, 128 * k : 128 * k + 128]
        pair = [mixed_re * cos + mixed_im * sin, mixed_im * cos - mixed_re * sin]
        both.append(jnp.concatenate(pair, axis=1).astype(bf16))
    waves = mm_t(second[grp], jnp.concatenate(both, axis=0))
    for k in range(8):
        u_all[8 * k : 8 * k + 8, :] = waves[:, 128 * k : 128 * k + 128]
    for k in range(ROLES):
        pair = [u_all[pl.ds(2 * k + c, 8, stride=8), :] for c in range(2)]
        u_out[k] = jnp.concatenate(pair, axis=1).astype(bf16)

    keep(u_out.at[role], s_in.at[slot], 2)

    def send_rows(i, _):
        device = near_peer(i)
        push(u_out.at[device[0]], s_in.at[slot], 2, device)
        return 0

    lax.fori_loop(0, 10, send_rows, 0)
    lax.fori_loop(11, NEAR, send_rows, 0)
    arrive(s_in, 2)

    for k in range(NEAR):
        arrived = s_in[k].astype(f32)
        for c in range(2):
            s_all[128 * c + 8 * k : 128 * c + 8 * k + 8, :] = arrived[:, 128 * c : 128 * c + 128]
    slots = lax.broadcasted_iota(jnp.int32, (1, KMAX), 1)
    total = [[jnp.zeros((8, 128), f32) for _ in range(4)] for _ in range(3)]
    def columns(k, p):
        return slice(KMAX * (NP_LOCAL * k + p), KMAX * (NP_LOCAL * k + p + 1))

    for k in range(REPS):
        predicted = [[], []]
        live = []
        for p in range(NP_LOCAL):
            row_block, _ = block_of(k, p, 128)
            rows = []
            for m in range(8):
                block = s_all[32 * m : 32 * m + 8, :]
                for h in range(1, 4):
                    at = slice(32 * m + 8 * h, 32 * m + 8 * h + 8)
                    block = jnp.where(row_block == h, s_all[at, :], block)
                rows.append(block)
            along = mm(jnp.concatenate(rows, axis=0).astype(bf16), kv_wide[:, columns(k, p)])
            ku_p = ku[:, columns(k, p)]
            for c in range(2):
                product = along[32 * c : 32 * c + 32] * ku_p
                predicted[c].append(jnp.sum(product, axis=0, keepdims=True))
            live.append(jnp.broadcast_to(counts[k, 0:1, p : p + 1], (1, KMAX)))
        alive = slots < jnp.concatenate(live, axis=0)
        for c in range(2):
            over = observed[k, c, 0] - jnp.concatenate(predicted[c], axis=0)
            left[k, c, 0] = jnp.where(alive, over, 0.0)
    for k, p in patches:
        cols = columns(k, p)
        row_block, col_block = block_of(k, p, 128)
        kv_p = kv[:, cols]
        weighted = [(kv_p * left[k, c, 0, p : p + 1, :]).astype(bf16) for c in range(2)]
        mine_u = ku[pl.ds(pl.multiple_of(8 * rep, 8), 8), cols].astype(bf16)
        both = mm_t(mine_u, jnp.concatenate(weighted + weighted, axis=0))
        turned = pltpu.roll(both, 32, 1)
        even = (lane // 32) % 2 == 0
        pieces = (
            (jnp.where(even, both, turned), lane // 32 == col_block - 1),
            (jnp.where(even, turned, both), lane // 32 == col_block - 1),
            (
                jnp.where((lane < 32) | (lane >= 96), both, turned),
                jnp.where(even, 0, 5) == col_block,
            ),
        )
        for j, (piece, inside) in enumerate(pieces):
            for h in range(4):
                here = jnp.where(row_block == h, 1, 0) * jnp.where(inside, 1, 0)
                total[j][h] = total[j][h] + jnp.where(here > 0, piece, 0.0)

    z_all[pl.ds(3, GRPS, stride=4), :] = jnp.zeros((GRPS, 128), f32)
    for k in range(3):
        z_all[pl.ds(k, GRPS, stride=4), :] = jnp.concatenate(total[k], axis=0)
    for k in range(GRPS):
        z_out[k] = z_all[4 * k : 4 * k + 4, :].astype(bf16)
    keep(z_out.at[grp], z_in.at[sub], 3)

    def send_owner(to):
        for k in range(ROLES):
            push(z_out.at[to], z_in.at[sub], 3, (lax.rem(role + k, ROLES), to, rep))

    def send_early(i, _):
        to = i

        @pl.when(to != grp)
        def _():
            push(z_out.at[to], z_in.at[sub], 3, (role, to, rep))

        for k in range(1, ROLES):
            push(z_out.at[to], z_in.at[sub], 3, (lax.rem(role + k, ROLES), to, rep))
        return 0

    lax.fori_loop(0, GRPS, send_early, 0)
    residual[...] = left[rep]
    arrive(z_in, 3)

    for k in range(C):
        z_all[4 * k : 4 * k + 4, :] = z_in[k].astype(f32)
    owned = [z_all[pl.ds(k, C, stride=4), :] for k in range(3)]
    edges = owned[2]
    column = lax.broadcasted_iota(jnp.int32, (C, 128), 1)
    subgrid = lax.broadcasted_iota(jnp.int32, (C, 128), 0)
    for c in range(2):
        side = pltpu.roll(edges, 96 if c == 0 else 32, 1)
        from_left = jnp.where((column < 32) & (subgrid > 0), pltpu.roll(side, 1, 0), 0.0)
        from_right = jnp.where((column >= 96) & (subgrid < C - 1), pltpu.roll(side, C - 1, 0), 0.0)
        returned[c] = (owned[c] + from_left + from_right).astype(bf16)

    drain(x_in, NEAR - 1, 0)
    drain(q_in, GRPS - 1, 1)
    drain(s_in, NEAR - 1, 2)
    drain(z_in, C - 1, 3)
    for k, held in enumerate(shared):
        drain(held, REPS - 1, 4 + k)


def flush(residual, returned, residual_out, returned_out, done):
    copies = [
        pltpu.make_async_copy(returned, returned_out, done.at[0]),
        pltpu.make_async_copy(residual, residual_out, done.at[1]),
    ]
    for copy in copies:
        copy.start()
    for copy in copies:
        copy.wait()


def local(facets, taper, kernel, observed, patch_pos, counts, vis_u, vis_v):
    vmem = pl.BlockSpec(memory_space=pltpu.VMEM)
    hbm = pl.BlockSpec(memory_space=pltpu.HBM)
    residual, returned = pl.pallas_call(
        body,
        out_shape=(
            pltpu.VMEM((2, 1, NP_LOCAL, KMAX), f32),
            pltpu.VMEM((2, C, C), bf16),
        ),
        in_specs=[hbm] * 13,
        out_specs=(vmem, vmem),
        scratch_shapes=[
            pltpu.VMEM((2, 32, F), bf16),
            pltpu.VMEM((1, F), f32),
            pltpu.VMEM((128, 256), bf16),
            pltpu.VMEM((32, 256), f32),
            pltpu.VMEM((256, 64), bf16),
            pltpu.VMEM((128, 256), f32),
            pltpu.VMEM((GRPS, 8, 256), bf16),
            pltpu.VMEM((1, KW), f32),
            pltpu.VMEM((REPS, 2, 1, NP_LOCAL, KMAX), f32),
            pltpu.VMEM((REPS, 1, NP_LOCAL), jnp.int32),
            pltpu.VMEM((REPS, 1, NP_LOCAL), jnp.int32),
            pltpu.VMEM((REPS, 1, NP_LOCAL, KMAX), jnp.int32),
            pltpu.VMEM((REPS, 1, NP_LOCAL, KMAX), jnp.int32),
            pltpu.VMEM((NEAR, 8, 128), bf16),
            pltpu.VMEM((NEAR, 8, 128), bf16),
            pltpu.VMEM((1, 8, 256), bf16),
            pltpu.VMEM((GRPS, 8, 256), bf16),
            pltpu.VMEM((16 * GRPS, 128), f32),
            pltpu.VMEM((64, 128), f32),
            pltpu.VMEM((ROLES, 8, 256), bf16),
            pltpu.VMEM((NEAR, 8, 256), bf16),
            pltpu.VMEM((4 * C, 128), f32),
            pltpu.VMEM((GRPS, 4, 128), bf16),
            pltpu.VMEM((C, 4, 128), bf16),
            pltpu.VMEM((2 * C, 128), f32),
            pltpu.VMEM((REPS, 2, 1, NP_LOCAL, KMAX), f32),
            pltpu.VMEM((PATCH, REPS * NP_LOCAL * KMAX), f32),
            pltpu.VMEM((PATCH, REPS * NP_LOCAL * KMAX), f32),
            pltpu.VMEM((C, REPS * NP_LOCAL * KMAX), bf16),
            pltpu.SemaphoreType.DMA((9,)),
            pltpu.SemaphoreType.DMA((9,)),
            pltpu.SemaphoreType.DMA((16,)),
        ],
        compiler_params=pltpu.CompilerParams(
            collective_id=0, has_side_effects=True
        ),
        name="cycle",
    )(facets, taper, *tables(), kernel[None], observed, patch_pos, counts, vis_u, vis_v)
    anywhere = pl.BlockSpec(memory_space=pl.ANY)
    residual, returned = pl.pallas_call(
        flush,
        out_shape=(
            jax.ShapeDtypeStruct((2, 1, NP_LOCAL, KMAX), f32),
            jax.ShapeDtypeStruct((2, C, C), bf16),
        ),
        in_specs=[vmem, vmem],
        out_specs=(anywhere, anywhere),
        scratch_shapes=[pltpu.SemaphoreType.DMA((2,))],
        compiler_params=pltpu.CompilerParams(vmem_limit_bytes=1 << 20),
        name="flush",
    )(residual, returned)
    return residual, returned.reshape(2, C, 1, C)


def solution(mesh):
    both = ("role", "grp")
    return jax.shard_map(
        local,
        mesh=mesh,
        in_specs=(
            P("role", None, ("grp", "rep"), None),
            P("role", None),
            P(),
            P(None, both, "rep", None),
            P(both, "rep"),
            P(both, "rep"),
            P(both, "rep", None),
            P(both, "rep", None),
        ),
        out_specs=(P(None, both, "rep", None), P(None, None, ("grp", "rep"), None)),
        check_vma=False,
    )
```
